128 devices in a mesh: dp: 8 (over y, x_hi), expert: 16 (over z, x_lo, core).
Axes of the slice: x: 4 (x_hi: 2, x_lo: 2; x = x_hi * 2 + x_lo), y: 4, z: 4, core: 2. Of those that a mesh axis runs over, the one named last changes fastest.
Arguments:
- expert_ids: int32 [4096, 8], P(('dp', 'expert')), may hold values from 0 to 15, all different within a row; in each aligned block of 32 rows (0 to 31, 32 to 63, ...) at most 20 rows name the same one
- expert_home: int32 [16], replicated, may hold values from 0 to 15, each once
- live_tokens: int32 [128], P(('dp', 'expert')), may hold values from 1 to 32, 3072 in all
- gate_weights: float32 [4096, 8], P(('dp', 'expert')), may hold values from 0.1 to 1
- output_grad: bfloat16 [4096, 7168], P(('dp', 'expert')), may hold values from -6 to 6
- saved_hidden: bfloat16 [4096, 8, 1024], P(('dp', 'expert')), may hold values from -2.5 to 2.5
- down_weight: bfloat16 [16, 1024, 7168], P('expert'), may hold values from -0.1875 to 0.1875
- dense_input: bfloat16 [4096, 7168], P(('dp', 'expert')), may hold values from -24 to 24
- latent_grad: bfloat16 [4096, 256], P(('dp', 'expert')), may hold values from -0.09375 to 0.09375
Outputs:
- hidden_grad: bfloat16 [4096, 8, 1024], P(('dp', 'expert'))
- expert_grad: float32 [16, 1024, 7168], P('expert', 'dp')
- dense_grad: float32 [7168, 256], P(('dp', 'expert'))
The draws below stay inside these ranges and needn't reach their ends.
Inputs may be any that keep to these rules, and one draw needn't show every extreme that they name: `expert_ids`: each row names 8 different experts. Among the rows of one device no expert is named more than 20 times, and on some devices one expert is named exactly 20 times. A permutation: expert e is held at index expert_home[e] of the expert axis, in every dp replica. `live_tokens`: entry i is the number of real tokens at the start of device i, in the order of the joined dp and expert axes; the rest are padding. Some device has all 32 real.
All inputs are finite; a program needn't handle non-finite values.
Results may differ from the reference program's by a relative error of at most 0.008.
Values may be sent and summed in bfloat16 or wider, within the bound.
A program may use at most 192 MiB of HBM per device.

```python
import math
import jax
import jax.numpy as jnp
import numpy as np
from jax import lax

D = 7168
KVR = 256
FFE = 1024
TOK_DEV = 32
EXPERTS = 16
TOPK = 8
CAP = 20
TOKENS = 4096
N_DP = 8
DEVICES = 128


def strengthened(result, own_key, source, target, shards_of, factor):
    owner, partner = [(jnp.arange(result.shape[position]) // (result.shape[position] // shards_of)).reshape([-1 if axis == position else 1 for axis in range(result.ndim)]) for position in (source, target)]
    chosen = jax.random.permutation(own_key, shards_of)[partner]
    strong = (owner == chosen) | (owner == (partner + shards_of // 2) % shards_of)
    return jnp.where(strong, factor * result, result)


def level_of(key, shape, split, low, top_value):
    gain = 1.0
    for dim, blocks in split:
        heights = jax.random.uniform(jax.random.fold_in(jax.random.fold_in(key, 6), dim), (blocks,), jnp.float32, low / len(split), top_value / len(split))
        gain = gain * jnp.repeat(jnp.exp(heights), shape[dim] // blocks).reshape((-1,) + (1,) * (len(shape) - 1 - dim))
    return gain


def profile(count, total, bound, skew):
    loads = [(1 << 20) // math.isqrt(standing ** skew) + 1 for standing in range(2, count + 1)]
    rest, given = total - bound - (count - 1), [1] * (count - 1)
    while rest > 0:
        movable = [i for i in range(count - 1) if given[i] < bound]
        mass, left = sum([loads[i] for i in movable]), rest
        for i in movable:
            addition = min(bound - given[i], max(1, left * loads[i] // mass), rest)
            given[i] = given[i] + addition
            rest = rest - addition
    return np.array([bound] + given)


def uneven(rng, amount, total, reach, lean):
    if amount == 2:
        one = jax.random.randint(rng, (), max(1, total - reach), min(reach, total - 1) + 1)
        return jnp.stack([one, total - one])
    sizes = jnp.asarray(profile(amount, total, reach, lean), jnp.int32)
    pairs = (amount - 1) // 2
    source_of, taker = sizes[1:1 + 2 * pairs:2], sizes[2:2 + 2 * pairs:2]
    room = jnp.minimum(source_of - 1, reach - taker)
    shifted = jax.random.randint(jax.random.fold_in(rng, 1), (pairs,), 0, 1 << 20) % (room + 1)
    sizes = sizes.at[1:1 + 2 * pairs:2].set(source_of - shifted).at[2:2 + 2 * pairs:2].set(taker + shifted)
    return sizes[jax.random.permutation(jax.random.fold_in(rng, 2), amount)]


def assign_block(own_key, own, number, rows, amount, top, limit, slope):
    ranking = jax.random.permutation(own_key, amount)
    crowded, ordinary = portions_of(amount, rows * top, limit, slope, True), portions_of(amount, rows * top, limit, slope, False)
    places = jnp.arange(amount)

    def named(lengths, turn):
        used = int((lengths > 0).sum())
        fixed = max(1, used // 4)
        shifted = fixed + (places - fixed + turn * (used - fixed)) % max(1, amount - fixed)
        return jnp.zeros((amount,), jnp.int32).at[ranking[jnp.where(places < fixed, places, shifted)]].set(jnp.asarray(lengths, jnp.int32))

    lengths = jnp.where(number % 4 == 0, named(crowded, number // 4), named(ordinary, number - number // 4 - 1))
    mixed = jax.random.permutation(jax.random.fold_in(own, 3), amount)
    giver, receiver = mixed[0:amount // 2 * 2:2], mixed[1:amount // 2 * 2:2]
    margin = jnp.minimum(lengths[giver] - 1, limit - lengths[receiver]) // 2
    margin = jnp.where((giver == ranking[0]) | (receiver == ranking[0]) | (lengths[receiver] == 0), 0, jnp.maximum(margin, 0))
    shifted = jax.random.randint(jax.random.fold_in(own, 4), (amount // 2,), 0, 1 << 20) % (margin + 1)
    lengths = lengths.at[giver].add(-shifted).at[receiver].add(shifted)
    items = jnp.searchsorted(jnp.cumsum(lengths), jnp.arange(rows * top), side="right").astype(jnp.int32)
    grid = items.reshape(top, rows).T
    grid = grid[jax.random.permutation(jax.random.fold_in(own, 1), rows)]
    turn = jax.random.randint(jax.random.fold_in(own, 2), (rows, 1), 0, top)
    return jnp.take_along_axis(grid, (jnp.arange(top)[None, :] + turn) % top, axis=1)


def portions_of(count, total, reach, slope, full):
    portions = [(1 << 20) // math.isqrt(grade ** slope) + 1 for grade in range(1, count + 1)]
    largest = reach if full else min(reach, max(-(-total // count), total * portions[0] // sum(portions)))
    least = 1 if total - largest >= count - 1 else 0
    holding, spare = [largest] + [least] * (count - 1), total - largest - least * (count - 1)
    while spare > 0:
        candidates = [i for i in range(1, count) if holding[i] < largest] or [i for i in range(1, count) if holding[i] < reach]
        mass, budget = sum([portions[i] for i in candidates]), spare
        for i in candidates:
            extra = min(reach - holding[i], max(1, budget * portions[i] // mass), spare)
            holding[i] = holding[i] + extra
            spare = spare - extra
    return np.array(holding)


def centred(own_key, dims, spread, reach, split=(), kind=jnp.bfloat16):
    drawn = spread * jax.random.normal(own_key, dims, jnp.float32)
    if split:
        drawn = drawn * level_of(own_key, dims, split, -0.22, 0.18)
    return jnp.clip(drawn, -reach, reach).astype(kind)


def gaussian_with(key, extent, width, bound, split, heavy, kind=jnp.bfloat16):
    array = width * jax.random.normal(key, extent, jnp.float32)
    if split:
        array = array * level_of(key, extent, split, -0.22, 0.18)
    return jnp.clip(strengthened(array, jax.random.fold_in(key, 3), *heavy), -bound, bound).astype(kind)


def setup_inputs(seed: int = 0) -> dict:
    seeds = jax.random.split(jax.random.key(seed), 10)
    expert_ids_keys = jax.random.split(jax.random.fold_in(seeds[0], 1), TOKENS // TOK_DEV)
    expert_ids_turns = jax.random.permutation(jax.random.fold_in(seeds[0], 3), TOKENS // TOK_DEV)
    expert_ids = jax.vmap(lambda own, number: assign_block(jax.random.fold_in(seeds[0], 2), own, number, TOK_DEV, EXPERTS, TOPK, CAP, 2))(expert_ids_keys, expert_ids_turns).reshape((TOKENS, TOPK))
    expert_home = jax.random.permutation(seeds[1], EXPERTS).astype(jnp.int32)
    live_tokens = uneven(seeds[2], DEVICES, DEVICES * TOK_DEV * 3 // 4, TOK_DEV, 2).astype(jnp.int32)
    gate_weights = jnp.clip(0.1 + 0.9 * jax.random.uniform(seeds[3], (TOKENS, TOPK), jnp.float32) ** level_of(seeds[3], (TOKENS, TOPK), ((0, 128),), -0.2, 0.2), 0.1, 1.0)
    output_grad = centred(seeds[4], (TOKENS, D), 0.5, 6.0, ((0, 128),))
    saved_hidden = gaussian_with(seeds[5], (TOKENS, TOPK, FFE), 0.1, 2.5, ((0, 128),), (0, 2, 128, 5.5))
    down_weight = centred(seeds[6], (EXPERTS, FFE, D), FFE ** -0.5, 0.1875, ((0, 16),))
    dense_input = gaussian_with(seeds[7], (TOKENS, D), 1.0, 24.0, ((0, 128),), (0, 1, 128, 5.5))
    latent_grad = centred(seeds[8], (TOKENS, KVR), TOKENS ** -0.5, 0.09375, ((0, 128),))
    return {"expert_ids": expert_ids, "expert_home": expert_home, "live_tokens": live_tokens, "gate_weights": gate_weights, "output_grad": output_grad, "saved_hidden": saved_hidden, "down_weight": down_weight, "dense_input": dense_input, "latent_grad": latent_grad}


def reference(expert_ids, expert_home, live_tokens, gate_weights, output_grad, saved_hidden, down_weight, dense_input, latent_grad):
    token_index = jnp.arange(TOK_DEV, dtype=jnp.int32)
    is_live = (token_index[None, :] < live_tokens[:, None]).reshape(TOKENS)
    masked_grad = jnp.where(is_live[:, None], latent_grad, jnp.zeros_like(latent_grad))
    dense_grad = jnp.dot(dense_input.T, masked_grad, preferred_element_type=jnp.float32)
    pair_home = expert_home[expert_ids]
    pair_scale = gate_weights * is_live[:, None].astype(jnp.float32)
    grad_wide = output_grad.astype(jnp.float32)

    def one_expert(carry, slot):
        chosen = pair_home == slot
        coefficient = jnp.sum(jnp.where(chosen, pair_scale, jnp.float32(0.0)), axis=1)
        gated = (grad_wide * coefficient[:, None]).astype(jnp.bfloat16)
        hidden_rows = jnp.sum(jnp.where(chosen[:, :, None], saved_hidden.astype(jnp.float32), jnp.float32(0.0)), axis=1)
        expert_weight = down_weight[slot]
        input_grad = jnp.dot(gated, expert_weight.T, preferred_element_type=jnp.float32).astype(jnp.bfloat16)
        carry = jnp.where(chosen[:, :, None], input_grad[:, None, :], carry)
        replica_hidden = hidden_rows.reshape(N_DP, TOKENS // N_DP, FFE)
        replica_grad = gated.astype(jnp.float32).reshape(N_DP, TOKENS // N_DP, D)
        partial_value = jnp.einsum("rtf,rtd->rfd", replica_hidden, replica_grad)
        summed = jnp.sum(partial_value, axis=0)
        return carry, summed

    start_grad = jnp.zeros((TOKENS, TOPK, FFE), jnp.bfloat16)
    hidden_grad, expert_grad = lax.scan(one_expert, start_grad, jnp.arange(EXPERTS, dtype=jnp.int32))
    return hidden_grad, expert_grad, dense_grad
```

```python
import functools

import jax
import jax.numpy as jnp
from jax import lax
from jax.experimental import pallas as pl
from jax.experimental.pallas import tpu as pltpu
from jax.sharding import Mesh
from jax.sharding import PartitionSpec as P

DP = ("y", "xh")
EXPERT = ("z", "xl", "c")
ALL = ("y", "xh", "z", "xl", "c")
MESH = pl.DeviceIdType.MESH
NY, NX, NZ, NCORE, NXH, NXL = 4, 4, 4, 2, 2, 2
BF = jnp.bfloat16
F32 = jnp.float32
N_CHUNK = 4


def kernel(
    g_hbm,
    hs_hbm,
    w_hbm,
    x_hbm,
    lat_hbm,
    r_out,
    eg_out,
    dg_out,
    gbuf,
    hbuf,
    ht,
    wbuf,
    acch,
    hret,
    rbuf,
    part,
    own,
    relay,
    recv_p,
    recv_m,
    xbuf,
    lbuf,
    dpart,
    drecv,
    a1_s,
    a1_r,
    a2_s,
    a2_r,
    b1_s,
    b1_r,
    b2_s,
    b2_r,
    dd_s,
    dd_r,
    h_s,
    h_r,
    rs_s,
    rs_r,
    hr_s,
    hr_r,
    dx_s,
    dx_r,
    dl_s,
    dl_r,
    ds_s,
    ds_r,
    loc,
    w_sem,
    o_sem,
):
    y = lax.axis_index("y")
    xh = lax.axis_index("xh")
    z = lax.axis_index("z")
    xl = lax.axis_index("xl")
    c = lax.axis_index("c")
    x = xh * NXL + xl
    slot = z * 4 + xl * 2 + c
    dp = y * 2 + xh
    tok = g_hbm.shape[0]
    half_tok = tok // 2
    chunk = gbuf.shape[-1]
    half = chunk // 2
    frows = ht.shape[0] // NY
    hrow = frows // 2
    hid = w_hbm.shape[0]
    dcols = xbuf.shape[-1]
    drows = drecv.shape[1]

    def up(v, k, n):
        return lax.rem(v + k, n)

    def at_x(v):
        return {"xh": v // NXL, "xl": lax.rem(v, NXL)}

    xp, xm, x2 = up(x, 1, NX), up(x, NX - 1, NX), up(x, 2, NX)
    zp, zm, z2 = up(z, 1, NZ), up(z, NZ - 1, NZ), up(z, 2, NZ)
    yp, ym = up(y, 1, NY), up(y, NY - 1, NY)
    dev_x = (at_x(xp), at_x(xm))
    dev_z = ({"z": zp}, {"z": zm})
    dev_y = ({"y": yp}, {"y": ym})
    sibling = {"c": 1 - c}
    sent = []

    def remote(src, dst, ss, rs, dev):
        return pltpu.make_async_remote_copy(
            src_ref=src, dst_ref=dst, send_sem=ss, recv_sem=rs, device_id=dev, device_id_type=MESH
        )

    def send(src, dst, ss, rs, dev):
        d = remote(src, dst, ss, rs, dev)
        d.start()
        sent.append(d)

    def arrived(ref, ss, rs, dev):
        remote(ref, ref, ss, rs, dev).wait_recv()

    def lanes(h):
        return pl.ds(h * half, half)

    def own_copy(ch):
        return pltpu.make_async_copy(
            g_hbm.at[:, pl.ds(ch * chunk, chunk)], gbuf.at[ch, x, c, z], loc.at[ch]
        )

    def s0(ch):
        own_copy(ch).start()
        for h in range(2):
            src = g_hbm.at[:, pl.ds(ch * chunk + h * half, half)]
            dst = gbuf.at[ch, x, c, z, :, lanes(h)]
            for s in range(2):
                i = h * 2 + s
                send(src, dst, a1_s.at[ch, i], a1_r.at[ch, i], (dev_x, dev_z)[h][s])

    rows_of = (pl.ds(0, half_tok), pl.ds(half_tok, half_tok))

    def s1(ch):
        for h in range(2):
            for s in range(2):
                i = h * 2 + s
                if h == 0:
                    blk = gbuf.at[ch, (xm, xp)[s], c, z]
                else:
                    blk = gbuf.at[ch, x, c, (zm, zp)[s]]
                dev = (dev_x, dev_z)[h][s]
                arrived(blk.at[:, lanes(h)], a1_s.at[ch, i], a1_r.at[ch, i], dev)
                ref = blk.at[rows_of[s], lanes(h)]
                send(ref, ref, a2_s.at[ch, i], a2_r.at[ch, i], dev)

    def line(ch, h, other):
        if h == 0:
            return gbuf.at[ch, :, c, other, :, lanes(0)]
        return gbuf.at[ch, other, c, :, :, lanes(1)]

    def line_half(ch, h, other, s):
        if h == 0:
            return gbuf.at[ch, :, c, other, rows_of[s], lanes(0)]
        return gbuf.at[ch, other, c, :, rows_of[s], lanes(1)]

    def s2(ch):
        own_copy(ch).wait()
        for h in range(2):
            for s in range(2):
                i = h * 2 + s
                blk = gbuf.at[ch, x2, c, z] if h == 0 else gbuf.at[ch, x, c, z2]
                arrived(
                    blk.at[rows_of[s], lanes(h)],
                    a2_s.at[ch, i],
                    a2_r.at[ch, i],
                    (dev_x, dev_z)[h][s],
                )
            ref = line(ch, h, (z, x)[h])
            for s in range(2):
                i = h * 2 + s
                send(ref, ref, b1_s.at[ch, i], b1_r.at[ch, i], (dev_z, dev_x)[h][s])
            send(ref, ref, dd_s.at[ch, h], dd_r.at[ch, h], sibling)

    def s3(ch):
        for h in range(2):
            for s in range(2):
                i = h * 2 + s
                other = ((zm, zp), (xm, xp))[h][s]
                dev = (dev_z, dev_x)[h][s]
                ref = line(ch, h, other)
                arrived(ref, b1_s.at[ch, i], b1_r.at[ch, i], dev)
                fwd = line_half(ch, h, other, s)
                send(fwd, fwd, b2_s.at[ch, i], b2_r.at[ch, i], dev)
                send(ref, ref, dd_s.at[ch, 2 + i], dd_r.at[ch, 2 + i], sibling)

    def s4(ch):
        for h in range(2):
            other = (z2, x2)[h]
            for s in range(2):
                i = h * 2 + s
                arrived(
                    line_half(ch, h, other, s),
                    b2_s.at[ch, i],
                    b2_r.at[ch, i],
                    (dev_z, dev_x)[h][s],
                )
            ref = line(ch, h, other)
            send(ref, ref, dd_s.at[ch, 6 + h], dd_r.at[ch, 6 + h], sibling)

    def s5(ch):
        for i in range(8):
            ref = line(ch, (0, 1, 0, 0, 1, 1, 0, 1)[i], z if (0, 1, 0, 0, 1, 1, 0, 1)[i] == 0 else x)
            arrived(ref, dd_s.at[ch, i], dd_r.at[ch, i], sibling)

    plane = [(i, j, k) for i in range(NX) for j in range(NCORE) for k in range(NZ)]

    def h_local():
        return pltpu.make_async_copy(hs_hbm.at[xh, slot], hbuf.at[x, c, z], loc.at[N_CHUNK])

    def h_send():
        h_local().start()
        for n, (i, j, k) in enumerate(plane):
            if n == 0:
                continue
            tx, tc, tz = up(x, i, NX), up(c, j, NCORE), up(z, k, NZ)
            t_slot = tz * 4 + lax.rem(tx, NXL) * 2 + tc
            send(
                hs_hbm.at[tx // NXL, t_slot],
                hbuf.at[x, c, z],
                h_s.at[n],
                h_r.at[n],
                {"xh": tx // NXL, "xl": lax.rem(tx, NXL), "z": tz, "c": tc},
            )

    def h_build():
        h_local().wait()
        for n in range(1, len(plane)):
            arrived(hbuf.at[x, c, z], h_s.at[n], h_r.at[n], sibling)
        for k in range(NY):
            yb = up(y, k, NY)
            for i in range(NX):
                blk = hbuf[i, :, :, :, pl.ds(pl.multiple_of(yb * frows, frows), frows)]
                n_tok = NCORE * NZ * tok
                ht[pl.ds(k * frows, frows), pl.ds(i * n_tok, n_tok)] = blk.reshape(n_tok, frows).T

    def w_copy(ch):
        return pltpu.make_async_copy(
            w_hbm.at[:, pl.ds(ch * chunk, chunk)], wbuf.at[ch % 2], w_sem.at[ch % 2]
        )

    def mm1(ch):
        def body(n, carry):
            col = pl.ds(pl.multiple_of(n * 256, 256), 256)
            g = gbuf[ch, :, :, :, :, col].reshape(NX * NCORE * NZ * tok, 256)
            r = jnp.dot(ht[...], g, preferred_element_type=F32)
            own[ch, :, col] = r[0:frows]
            for k in range(1, NY):
                part[ch, k, :, col] = r[k * frows : (k + 1) * frows].astype(BF)
            return carry

        lax.fori_loop(0, chunk // 256, body, 0)

    def mm2(ch):
        w_copy(ch).wait()

        def body(n, carry):
            row = pl.ds(pl.multiple_of(n * 256, 256), 256)
            g = gbuf[ch, pl.ds(xh * NXL, NXL)].reshape(NXL * NCORE * NZ * tok, chunk)
            r = lax.dot_general(
                g, wbuf[ch % 2, row, :], (((1,), (1,)), ((), ())), preferred_element_type=F32
            )
            if ch == 0:
                acch[:, row] = r
            else:
                acch[:, row] = acch[:, row] + r
            return carry

        lax.fori_loop(0, hid // 256, body, 0)
        if ch + 2 < N_CHUNK:
            w_copy(ch + 2).start()

    row_a, row_b = pl.ds(0, hrow), pl.ds(hrow, hrow)

    def r0(ch):
        send(part.at[ch, 2, row_b], relay.at[ch, 0], rs_s.at[ch, 0], rs_r.at[ch, 0], dev_y[0])
        send(part.at[ch, 2, row_a], relay.at[ch, 1], rs_s.at[ch, 1], rs_r.at[ch, 1], dev_y[1])
        send(part.at[ch, 1, row_a], recv_m.at[ch, row_a], rs_s.at[ch, 2], rs_r.at[ch, 2], dev_y[0])
        send(part.at[ch, 3, row_b], recv_p.at[ch, row_b], rs_s.at[ch, 3], rs_r.at[ch, 3], dev_y[1])

    def r1(ch):
        arrived(relay.at[ch, 0], rs_s.at[ch, 0], rs_r.at[ch, 0], dev_y[0])
        part[ch, 1, row_b] = (part[ch, 1, row_b].astype(F32) + relay[ch, 0].astype(F32)).astype(BF)
        send(part.at[ch, 1, row_b], recv_m.at[ch, row_b], rs_s.at[ch, 4], rs_r.at[ch, 4], dev_y[0])
        arrived(relay.at[ch, 1], rs_s.at[ch, 1], rs_r.at[ch, 1], dev_y[1])
        part[ch, 3, row_a] = (part[ch, 3, row_a].astype(F32) + relay[ch, 1].astype(F32)).astype(BF)
        send(part.at[ch, 3, row_a], recv_p.at[ch, row_a], rs_s.at[ch, 5], rs_r.at[ch, 5], dev_y[1])

    def out_copy(ch):
        return pltpu.make_async_copy(
            own.at[ch], eg_out.at[:, pl.ds(ch * chunk, chunk)], o_sem.at[ch]
        )

    def r2(ch):
        for i in range(2, 6):
            arrived(relay.at[ch, 0], rs_s.at[ch, i], rs_r.at[ch, i], dev_y[i % 2])
        own[ch] = own[ch] + (recv_m[ch].astype(F32) + recv_p[ch].astype(F32))
        out_copy(ch).start()

    group = [(i, j, k) for i in range(NXL) for j in range(NCORE) for k in range(NZ)]

    def hr_send():
        hret[...] = acch[...].astype(BF).reshape(hret.shape)
        for n, (i, j, k) in enumerate(group):
            if n == 0:
                continue
            tx, tc, tz = up(xl, i, NXL), up(c, j, NCORE), up(z, k, NZ)
            send(
                hret.at[tx, tc, tz],
                rbuf.at[slot],
                hr_s.at[n],
                hr_r.at[n],
                {"xl": tx, "z": tz, "c": tc},
            )
        rbuf[slot] = hret[xl, c, z]

    def r_copy():
        return pltpu.make_async_copy(rbuf, r_out, o_sem.at[N_CHUNK])

    def hr_wait():
        for n in range(1, len(group)):
            arrived(rbuf.at[slot], hr_s.at[n], hr_r.at[n], sibling)
        r_copy().start()

    owners = [(i, j) for i in range(NY) for j in range(NXH)]

    def d_local():
        return (
            pltpu.make_async_copy(
                x_hbm.at[:, pl.ds(pl.multiple_of(dp * dcols, 128), dcols)],
                xbuf.at[dp],
                loc.at[N_CHUNK + 1],
            ),
            pltpu.make_async_copy(lat_hbm, lbuf.at[dp], loc.at[N_CHUNK + 2]),
        )

    def d0():
        for d in d_local():
            d.start()
        for n, (i, j) in enumerate(owners):
            if n == 0:
                continue
            ty, th = up(y, i, NY), up(xh, j, NXH)
            td = ty * 2 + th
            dev = {"y": ty, "xh": th}
            send(
                x_hbm.at[:, pl.ds(pl.multiple_of(td * dcols, 128), dcols)],
                xbuf.at[dp],
                dx_s.at[n],
                dx_r.at[n],
                dev,
            )
            send(lat_hbm, lbuf.at[dp], dl_s.at[n], dl_r.at[n], dev)

    def d1():
        for d in d_local():
            d.wait()
        for n in range(1, len(owners)):
            arrived(xbuf.at[dp], dx_s.at[n], dx_r.at[n], sibling)
            arrived(lbuf.at[dp], dl_s.at[n], dl_r.at[n], sibling)
        n_tok = len(owners) * tok

        def body(n, carry):
            col = pl.ds(pl.multiple_of(n * 128, 128), 128)
            xt = xbuf[:, :, col].reshape(n_tok, 128).T
            dpart[col, :] = jnp.dot(
                xt, lbuf[...].reshape(n_tok, lbuf.shape[-1]), preferred_element_type=F32
            )
            return carry

        lax.fori_loop(0, dcols // 128, body, 0)
        for n, (i, j, k) in enumerate(group):
            if n == 0:
                continue
            tx, tc, tz = up(xl, i, NXL), up(c, j, NCORE), up(z, k, NZ)
            ts = tz * 4 + tx * 2 + tc
            send(
                dpart.at[pl.ds(pl.multiple_of(ts * drows, 8), drows)],
                drecv.at[slot],
                ds_s.at[n],
                ds_r.at[n],
                {"xl": tx, "z": tz, "c": tc},
            )
        drecv[slot] = dpart[pl.ds(pl.multiple_of(slot * drows, 8), drows)]

    def d2():
        for n in range(1, len(group)):
            arrived(drecv.at[slot], ds_s.at[n], ds_r.at[n], sibling)
        total = drecv[0]
        for n in range(1, len(group)):
            total = total + drecv[n]
        dg_out[...] = total

    w_copy(0).start()
    w_copy(1).start()
    s0(0)
    d0()
    s0(1)
    s1(0)
    s2(0)
    h_send()
    s1(1)
    s3(0)
    s2(1)
    s0(2)
    s0(3)
    s4(0)
    s3(1)
    h_build()
    s1(2)
    s2(2)
    s5(0)
    mm1(0)
    r0(0)
    s4(1)
    s3(2)
    s1(3)
    s2(3)
    mm2(0)
    s5(1)
    mm1(1)
    r0(1)
    s4(2)
    s3(3)
    r1(0)
    mm2(1)
    s5(2)
    mm1(2)
    r0(2)
    s4(3)
    d1()
    r1(1)
    mm2(2)
    s5(3)
    mm1(3)
    r0(3)
    mm2(3)
    hr_send()
    r2(0)
    r1(2)
    r2(1)
    d2()
    hr_wait()
    r1(3)
    r2(2)
    r2(3)
    for ch in range(N_CHUNK):
        out_copy(ch).wait()
    r_copy().wait()
    for d in sent:
        d.wait_send()


def exchange(g, hs, w, xin, lat):
    tok, d = g.shape
    chunk = d // N_CHUNK
    hid = w.shape[0]
    n_plane = NX * NCORE * NZ
    frows = hid // NXH // NY
    kvr = lat.shape[1]
    drows = d // 128
    dma = pltpu.SemaphoreType.DMA
    any_spec = pl.BlockSpec(memory_space=pl.ANY)
    v = pltpu.VMEM
    scratch = [
        v((N_CHUNK, NX, NCORE, NZ, tok, chunk), BF),
        v((NX, NCORE, NZ, tok, hid // NXH), BF),
        v((hid // NXH, n_plane * tok), BF),
        v((2, hid, chunk), BF),
        v((16 * tok, hid), F32),
        v((NXL, NCORE, NZ, tok, hid), BF),
        v((16, tok, hid), BF),
        v((N_CHUNK, NY, frows, chunk), BF),
        v((N_CHUNK, frows, chunk), F32),
        v((N_CHUNK, 2, frows // 2, chunk), BF),
        v((N_CHUNK, frows, chunk), BF),
        v((N_CHUNK, frows, chunk), BF),
        v((8, tok, d // 8), BF),
        v((8, tok, kvr), BF),
        v((d // 8, kvr), F32),
        v((16, drows, kvr), F32),
    ]
    sems = []
    for shape in ((N_CHUNK, 4), (N_CHUNK, 4), (N_CHUNK, 4), (N_CHUNK, 4), (N_CHUNK, 8), (32,), (N_CHUNK, 6), (16,), (8,), (8,), (16,)):
        sems += [dma(shape), dma(shape)]
    sems += [dma((N_CHUNK + 3,)), dma((2,)), dma((N_CHUNK + 1,))]
    return pl.pallas_call(
        kernel,
        out_shape=(
            jax.ShapeDtypeStruct((16, tok, hid), BF),
            jax.ShapeDtypeStruct((frows, d), F32),
            jax.ShapeDtypeStruct((drows, kvr), F32),
        ),
        in_specs=[any_spec] * 5,
        out_specs=(any_spec, any_spec, pl.BlockSpec(memory_space=pltpu.VMEM)),
        scratch_shapes=scratch + sems,
        compiler_params=pltpu.CompilerParams(
            has_side_effects=True, vmem_limit_bytes=62 * 1024 * 1024
        ),
        name="exchange",
    )(g, hs, w, xin, lat)


def on_device(
    expert_ids,
    expert_home,
    live_tokens,
    gate_weights,
    output_grad,
    saved_hidden,
    down_weight,
    dense_input,
    latent_grad,
):
    tok, topk = expert_ids.shape
    hid = saved_hidden.shape[2]
    n_slot = 16
    is_live = jnp.arange(tok, dtype=jnp.int32) < live_tokens[0]
    masked = jnp.where(is_live[:, None], latent_grad, jnp.zeros_like(latent_grad))
    ids = expert_ids.reshape(tok * topk)
    table = ids[:, None] == jnp.arange(n_slot, dtype=jnp.int32)[None, :]
    home = jnp.sum(jnp.where(table, expert_home[None, :], 0), axis=1)
    token = jnp.arange(tok * topk, dtype=jnp.int32) // topk
    place = home * tok + token
    pick = (jnp.arange(n_slot * tok, dtype=jnp.int32)[:, None] == place[None, :]).astype(BF)
    scale = (gate_weights * is_live[:, None].astype(F32)).reshape(tok * topk)
    scaled = (saved_hidden.reshape(tok * topk, hid).astype(F32) * scale[:, None]).astype(BF)
    halves = scaled.reshape(tok * topk, NY, NXH, hid // 8)
    hs = jnp.stack(
        [
            jnp.dot(
                pick,
                halves[:, :, j].reshape(tok * topk, hid // 2),
                preferred_element_type=F32,
            ).astype(BF)
            for j in range(NXH)
        ]
    ).reshape(NXH, n_slot, tok, hid // 2)
    r, eg, dg = exchange(output_grad, hs, down_weight[0], dense_input, masked)
    back = lax.dot_general(
        pick, r.reshape(n_slot * tok, hid), (((0,), (0,)), ((), ())), preferred_element_type=F32
    )
    hg = (back * scale[:, None]).astype(BF).reshape(tok, topk, hid)
    return hg, eg[None], dg


def solution(mesh):
    torus = Mesh(mesh.devices.reshape(4, 2, 4, 2, 2), ALL)
    in_specs = (
        P(ALL, None),
        P(),
        P(ALL),
        P(ALL, None),
        P(ALL, None),
        P(ALL, None, None),
        P(EXPERT, None, None),
        P(ALL, None),
        P(ALL, None),
    )
    out_specs = (P(ALL, None, None), P(EXPERT, DP, None), P(ALL, None))
    return jax.shard_map(
        on_device, mesh=torus, in_specs=in_specs, out_specs=out_specs, check_vma=False
    )
```

```python
import jax
import jax.numpy as jnp
from jax import lax
from jax.experimental import pallas as pl
from jax.experimental.pallas import tpu as pltpu
from jax.sharding import Mesh
from jax.sharding import PartitionSpec as P

DP = ("y", "xh")
EXPERT = ("z", "xl", "c")
ALL = ("y", "xh", "z", "xl", "c")
MESH = pl.DeviceIdType.MESH
NY, NX, NZ, NCORE, NXH, NXL = 4, 4, 4, 2, 2, 2
N_SLOT = 16
BF = jnp.bfloat16
F32 = jnp.float32
WIDTHS = (768, 1280, 1536, 1792, 1792)
N_CHUNK = len(WIDTHS)
STARTS = tuple(sum(WIDTHS[:i]) for i in range(N_CHUNK))
PLANE = [(i, j, k) for i in range(NX) for j in range(NCORE) for k in range(NZ)]
GROUP = [(i, j, k) for i in range(NXL) for j in range(NCORE) for k in range(NZ)]
OWNERS = [(i, j) for i in range(NY) for j in range(NXH)]


def up(v, k, n):
    return lax.rem(v + k, n)


def kernel(names, *all_refs):
    r = dict(zip(names, all_refs))
    ids, home, live, gates, lat = (r[k] for k in ("ids", "home", "live", "gates", "lat"))
    g_hbm, sv_hbm, w_hbm, x_hbm = (r[k] for k in ("g", "sv", "w", "x"))
    hg_out, eg_out, dg_out = r["hg_out"], r["eg_out"], r["dg_out"]
    gbuf, part, relay, recv_p, recv_m = (
        [r[k + str(i)] for i in range(N_CHUNK)] for k in ("gbuf", "part", "relay", "recv_p", "recv_m")
    )
    hs, hbuf, ht, wbuf, acch, hret, rbuf = (
        r[k] for k in ("hs", "hbuf", "ht", "wbuf", "acch", "hret", "rbuf")
    )
    saved, pick, pick_t, coef, flip = (r[k] for k in ("saved", "pick", "pick_t", "coef", "flip"))
    xbuf, lsend, lbuf, dpart, dsend, drecv = (
        r[k] for k in ("xbuf", "lsend", "lbuf", "dpart", "dsend", "drecv")
    )

    y = lax.axis_index("y")
    xh = lax.axis_index("xh")
    z = lax.axis_index("z")
    xl = lax.axis_index("xl")
    c = lax.axis_index("c")
    x = xh * NXL + xl
    slot = z * 4 + xl * 2 + c
    dp = y * 2 + xh
    tok = g_hbm.shape[0]
    half_tok = tok // 2
    topk = ids.shape[0]
    pairs = tok * topk
    frows = ht.shape[0] // NY
    hrow = frows // 2
    hid = w_hbm.shape[0]
    dcols = xbuf.shape[-1]
    drows = drecv.shape[1]
    rows_of = (pl.ds(0, half_tok), pl.ds(half_tok, half_tok))

    def at_x(v):
        return {"xh": v // NXL, "xl": lax.rem(v, NXL)}

    xp, xm, x2 = up(x, 1, NX), up(x, NX - 1, NX), up(x, 2, NX)
    zp, zm, z2 = up(z, 1, NZ), up(z, NZ - 1, NZ), up(z, 2, NZ)
    yp, ym = up(y, 1, NY), up(y, NY - 1, NY)
    dev_x = (at_x(xp), at_x(xm), at_x(x2))
    dev_z = ({"z": zp}, {"z": zm}, {"z": z2})
    dev_y = ({"y": yp}, {"y": ym})
    sibling = {"c": 1 - c}
    sent = []

    def sems(name, *at):
        return r[name + "_s"].at[at], r[name + "_r"].at[at]

    def remote(src, dst, pair, dev):
        return pltpu.make_async_remote_copy(
            src_ref=src,
            dst_ref=dst,
            send_sem=pair[0],
            recv_sem=pair[1],
            device_id=dev,
            device_id_type=MESH,
        )

    def send(src, dst, pair, dev):
        d = remote(src, dst, pair, dev)
        d.start()
        sent.append(d)

    def arrived(ref, pair, dev):
        remote(ref, ref, pair, dev).wait_recv()

    def plane_dev(n):
        i, j, k = PLANE[n]
        tx, tc, tz = up(x, i, NX), up(c, j, NCORE), up(z, k, NZ)
        return tx, tc, tz, {"xh": tx // NXL, "xl": lax.rem(tx, NXL), "z": tz, "c": tc}

    barrier = pltpu.get_barrier_semaphore()

    def greet():
        for n in range(1, len(PLANE)):
            pl.semaphore_signal(barrier, inc=1, device_id=plane_dev(n)[3], device_id_type=MESH)
        for i, j in OWNERS:
            if i:
                dev = {"y": up(y, i, NY), "xh": up(xh, j, NXH)}
                pl.semaphore_signal(barrier, inc=1, device_id=dev, device_id_type=MESH)

    def bar():
        pl.semaphore_wait(barrier, len(PLANE) - 1 + 2 * (NY - 1))

    def own_copy(ch):
        return pltpu.make_async_copy(
            g_hbm.at[:, pl.ds(STARTS[ch], WIDTHS[ch])], gbuf[ch].at[x, c, z], r["loc"].at[ch]
        )

    def saved_copy():
        return pltpu.make_async_copy(sv_hbm, saved, r["loc"].at[N_CHUNK])

    def h_local():
        return pltpu.make_async_copy(hs.at[xh, slot], hbuf.at[x, c, z], r["loc"].at[N_CHUNK + 1])

    def d_local():
        return pltpu.make_async_copy(
            x_hbm.at[:, pl.ds(pl.multiple_of(dp * dcols, 128), dcols)],
            xbuf.at[dp],
            r["loc"].at[N_CHUNK + 2],
        )

    def w_copy(ch):
        return pltpu.make_async_copy(
            w_hbm.at[:, pl.ds(STARTS[ch], WIDTHS[ch])],
            wbuf.at[ch % 2, :, pl.ds(0, WIDTHS[ch])],
            r["w_sem"].at[ch % 2],
        )

    def prep():
        homes = jnp.zeros(ids.shape, F32)
        for e in range(N_SLOT):
            homes = jnp.where(ids[...] == e, home[e].astype(F32), homes)
        is_live = lax.broadcasted_iota(jnp.int32, ids.shape, 1) < live[0]
        flip[...] = jnp.zeros_like(flip)
        flip[0, 0:topk, 0:tok] = homes
        flip[1, 0:topk, 0:tok] = jnp.where(is_live, gates[...], jnp.zeros_like(gates))
        home_t = flip[0].T[0:tok]
        scale_t = flip[1].T[0:tok]
        lane = lax.broadcasted_iota(jnp.int32, (128, pairs), 1)
        row = lax.broadcasted_iota(jnp.int32, (128, pairs), 0)
        spread = jnp.where(lax.rem(lane, topk) == row, 1.0, 0.0).astype(BF)
        wide = jnp.dot(home_t.astype(BF), spread, preferred_element_type=F32)
        lane = lax.broadcasted_iota(jnp.int32, (tok, pairs), 1)
        row = lax.broadcasted_iota(jnp.int32, (tok, pairs), 0)
        wide = jnp.where(lane // topk == row, wide, -1.0)
        column = lax.broadcasted_iota(jnp.int32, (tok, 128), 1)
        for s in range(N_SLOT):
            pick[s] = jnp.where(wide == float(s), 1.0, 0.0).astype(BF)
            mine = jnp.where((home_t == float(s)) & (column < topk), scale_t, 0.0)
            coef[s] = jnp.broadcast_to(jnp.sum(mine, axis=1, keepdims=True), (tok, 128))
        token = lax.broadcasted_iota(jnp.int32, lat.shape, 0)
        lsend[...] = jnp.where(token < live[0], lat[...], jnp.zeros_like(lat))
        saved_copy().wait()
        table = pick[...].reshape(N_SLOT * tok, pairs)
        scale = coef[...].reshape(N_SLOT * tok, 128)
        for n in range(NY):
            rows = jnp.dot(table, saved[:, n * 256 : (n + 1) * 256], preferred_element_type=F32)
            for j in range(NXH):
                scaled = (rows[:, j * frows : (j + 1) * frows] * scale).astype(BF)
                hs[j, :, :, n * frows : (n + 1) * frows] = scaled.reshape(N_SLOT, tok, frows)

    def lanes(ch, h):
        return pl.ds(h * (WIDTHS[ch] // 2), WIDTHS[ch] // 2)

    def direct(ch):
        return ch == 0

    def s0(ch):
        own_copy(ch).wait()
        for h in range(2):
            ref = gbuf[ch].at[x, c, z, :, lanes(ch, h)]
            for s in range(3 if direct(ch) else 2):
                send(ref, ref, sems("a1", ch, h * 3 + s), (dev_x, dev_z)[h][s])

    def s1(ch):
        for h in range(2):
            for s in range(2):
                if h == 0:
                    blk = gbuf[ch].at[(xm, xp)[s], c, z]
                else:
                    blk = gbuf[ch].at[x, c, (zm, zp)[s]]
                dev = (dev_x, dev_z)[h][s]
                arrived(blk.at[:, lanes(ch, h)], sems("a1", ch, h * 3 + s), dev)
                ref = blk.at[rows_of[s], lanes(ch, h)]
                send(ref, ref, sems("a2", ch, h * 2 + s), dev)

    def line(ch, h, other):
        if h == 0:
            return gbuf[ch].at[:, c, other, :, lanes(ch, 0)]
        return gbuf[ch].at[other, c, :, :, lanes(ch, 1)]

    def line_half(ch, h, other, s):
        if h == 0:
            return gbuf[ch].at[:, c, other, rows_of[s], lanes(ch, 0)]
        return gbuf[ch].at[other, c, :, rows_of[s], lanes(ch, 1)]

    def s2(ch):
        for h in range(2):
            dev = (dev_x, dev_z)[h]
            blk = gbuf[ch].at[x2, c, z] if h == 0 else gbuf[ch].at[x, c, z2]
            if direct(ch):
                for s in range(3):
                    arrived(blk.at[:, lanes(ch, h)], sems("a1", ch, h * 3 + s), dev[s])
            else:
                for s in range(2):
                    arrived(blk.at[rows_of[s], lanes(ch, h)], sems("a2", ch, h * 2 + s), dev[s])
            ref = line(ch, h, (z, x)[h])
            for s in range(2):
                send(ref, ref, sems("b1", ch, h * 2 + s), (dev_z, dev_x)[h][s])
            send(ref, ref, sems("dd", ch, h), sibling)

    def s3(ch):
        for h in range(2):
            for s in range(2):
                i = h * 2 + s
                other = ((zm, zp), (xm, xp))[h][s]
                dev = (dev_z, dev_x)[h][s]
                ref = line(ch, h, other)
                arrived(ref, sems("b1", ch, i), dev)
                fwd = line_half(ch, h, other, s)
                send(fwd, fwd, sems("b2", ch, i), dev)
                send(ref, ref, sems("dd", ch, 2 + i), sibling)

    def s4(ch):
        for h in range(2):
            other = (z2, x2)[h]
            for s in range(2):
                dev = (dev_z, dev_x)[h][s]
                arrived(line_half(ch, h, other, s), sems("b2", ch, h * 2 + s), dev)
            ref = line(ch, h, other)
            send(ref, ref, sems("dd", ch, 6 + h), sibling)

    def s5(ch):
        for i, h in enumerate((0, 1, 0, 0, 1, 1, 0, 1)):
            arrived(line(ch, h, (z, x)[h]), sems("dd", ch, i), sibling)

    def h_send(first, last):
        if first == 0:
            h_local().start()
        for m in range(first, last):
            n = ((m + 1) * 11) % len(PLANE)
            tx, tc, tz, dev = plane_dev(n)
            t_slot = tz * 4 + lax.rem(tx, NXL) * 2 + tc
            send(hs.at[tx // NXL, t_slot], hbuf.at[x, c, z], sems("h", n), dev)

    def h_build():
        h_local().wait()
        for n in range(1, len(PLANE)):
            arrived(hbuf.at[x, c, z], sems("h", n), sibling)
        n_tok = NCORE * NZ * tok
        for k in range(NY):
            col = pl.ds(pl.multiple_of(up(y, k, NY) * frows, frows), frows)
            for i in range(NX):
                blk = hbuf[i, :, :, :, col].reshape(n_tok, frows)
                ht[pl.ds(k * frows, frows), pl.ds(i * n_tok, n_tok)] = blk.T

    def mm1(ch):
        def body(n, carry):
            col = pl.ds(pl.multiple_of(n * 256, 256), 256)
            g = gbuf[ch][:, :, :, :, col].reshape(len(PLANE) * tok, 256)
            p = jnp.dot(ht[...], g, preferred_element_type=F32)
            eg_out[:, pl.ds(pl.multiple_of(STARTS[ch] + n * 256, 256), 256)] = p[0:frows]
            for k in range(1, NY):
                part[ch][k - 1, :, col] = p[k * frows : (k + 1) * frows].astype(BF)
            return carry

        lax.fori_loop(0, WIDTHS[ch] // 256, body, 0)

    def mm2(ch):
        w_copy(ch).wait()

        def body(n, carry):
            row = pl.ds(pl.multiple_of(n * 256, 256), 256)
            g = gbuf[ch][pl.ds(xh * NXL, NXL)].reshape(len(GROUP) * tok, WIDTHS[ch])
            w = wbuf[ch % 2, row, pl.ds(0, WIDTHS[ch])]
            p = lax.dot_general(g, w, (((1,), (1,)), ((), ())), preferred_element_type=F32)
            if ch == 0:
                acch[:, row] = p
            else:
                acch[:, row] = acch[:, row] + p
            return carry

        lax.fori_loop(0, hid // 256, body, 0)
        if ch + 2 < N_CHUNK:
            w_copy(ch + 2).start()

    row_a, row_b = pl.ds(0, hrow), pl.ds(hrow, hrow)

    def r0(ch):
        p = part[ch]
        send(p.at[1, row_b], relay[ch].at[0], sems("rs", ch, 0), dev_y[0])
        send(p.at[1, row_a], relay[ch].at[1], sems("rs", ch, 1), dev_y[1])
        send(p.at[0, row_a], recv_m[ch].at[row_a], sems("rs", ch, 2), dev_y[0])
        send(p.at[2, row_b], recv_p[ch].at[row_b], sems("rs", ch, 3), dev_y[1])

    def r1(ch):
        p = part[ch]
        arrived(relay[ch].at[0], sems("rs", ch, 0), dev_y[0])
        p[0, row_b] = (p[0, row_b].astype(F32) + relay[ch][0].astype(F32)).astype(BF)
        send(p.at[0, row_b], recv_m[ch].at[row_b], sems("rs", ch, 4), dev_y[0])
        arrived(relay[ch].at[1], sems("rs", ch, 1), dev_y[1])
        p[2, row_a] = (p[2, row_a].astype(F32) + relay[ch][1].astype(F32)).astype(BF)
        send(p.at[2, row_a], recv_p[ch].at[row_a], sems("rs", ch, 5), dev_y[1])

    def r2(ch):
        for i in range(2, 6):
            arrived(relay[ch].at[0], sems("rs", ch, i), dev_y[i % 2])
        col = pl.ds(STARTS[ch], WIDTHS[ch])
        eg_out[:, col] = eg_out[:, col] + (recv_m[ch][...].astype(F32) + recv_p[ch][...].astype(F32))

    def group_dev(n):
        i, j, k = GROUP[n]
        tx, tc, tz = up(xl, i, NXL), up(c, j, NCORE), up(z, k, NZ)
        return tx, tc, tz, {"xl": tx, "z": tz, "c": tc}

    def hr_send():
        hret[...] = acch[...].astype(BF).reshape(hret.shape)
        for n in range(1, len(GROUP)):
            tx, tc, tz, dev = group_dev(n)
            send(hret.at[tx, tc, tz], rbuf.at[slot], sems("hr", n), dev)
        rbuf[slot] = hret[xl, c, z]

    def table_flip():
        pick_t[...] = pick[...].reshape(N_SLOT * tok, pairs).T

    def hr_wait():
        for n in range(1, len(GROUP)):
            arrived(rbuf.at[slot], sems("hr", n), sibling)
        scale = coef[...].reshape(N_SLOT * tok, 128)
        for n in range(hid // 256):
            halves = []
            for j in range(2):
                rows = rbuf[:, :, n * 256 + j * 128 : n * 256 + (j + 1) * 128]
                rows = rows.reshape(N_SLOT * tok, 128).astype(F32) * scale
                halves.append(rows.astype(BF))
            rows = jnp.concatenate(halves, axis=1)
            back = jnp.dot(pick_t[...], rows, preferred_element_type=F32)
            hg_out[:, n * 256 : (n + 1) * 256] = back.astype(BF)

    def d0(both):
        if not both:
            d_local().start()
            lbuf[dp] = lsend[...]
        for n, (i, j) in enumerate(OWNERS):
            if n == 0 or j != both:
                continue
            ty, th = up(y, i, NY), up(xh, j, NXH)
            td = ty * 2 + th
            dev = {"y": ty, "xh": th}
            send(
                x_hbm.at[:, pl.ds(pl.multiple_of(td * dcols, 128), dcols)],
                xbuf.at[dp],
                sems("dx", n),
                dev,
            )
            send(lsend, lbuf.at[dp], sems("dl", n), dev)

    def d1():
        d_local().wait()
        for n in range(1, len(OWNERS)):
            arrived(xbuf.at[dp], sems("dx", n), sibling)
            arrived(lbuf.at[dp], sems("dl", n), sibling)
        n_tok = len(OWNERS) * tok

        def body(n, carry):
            col = pl.ds(pl.multiple_of(n * 128, 128), 128)
            xt = xbuf[:, :, col].reshape(n_tok, 128).T
            dpart[col, :] = jnp.dot(
                xt, lbuf[...].reshape(n_tok, lbuf.shape[-1]), preferred_element_type=F32
            )
            return carry

        lax.fori_loop(0, dcols // 128, body, 0)
        for n in range(N_SLOT):
            dsend[n] = dpart[n * drows : (n + 1) * drows].astype(BF)
        for n in range(1, len(GROUP)):
            tx, tc, tz, dev = group_dev(n)
            send(dsend.at[tz * 4 + tx * 2 + tc], drecv.at[slot], sems("ds", n), dev)
        drecv[slot] = dsend[slot]

    def d2():
        for n in range(1, len(GROUP)):
            arrived(drecv.at[slot], sems("ds", n), sibling)
        mine = dpart[pl.ds(pl.multiple_of(slot * drows, 8), drows)]
        total = mine - drecv[slot].astype(F32)
        for n in range(len(GROUP)):
            total = total + drecv[n].astype(F32)
        dg_out[...] = total

    greet()
    saved_copy().start()
    own_copy(0).start()
    own_copy(1).start()
    own_copy(2).start()
    own_copy(3).start()
    own_copy(4).start()
    w_copy(0).start()
    w_copy(1).start()
    prep()
    bar()
    s0(0)
    h_send(0, 7)
    s2(0)
    s0(1)
    h_send(7, 15)
    s3(0)
    h_send(15, 31)
    s1(1)
    s4(0)
    s2(1)
    s0(2)
    table_flip()
    h_build()
    s5(0)
    mm1(0)
    r0(0)
    d0(0)
    s0(3)
    s0(4)
    s1(2)
    s3(1)
    s2(2)
    s4(1)
    mm2(0)
    s1(3)
    s5(1)
    mm1(1)
    r0(1)
    s3(2)
    s2(3)
    s1(4)
    s4(2)
    mm2(1)
    r1(0)
    s3(3)
    s2(4)
    s5(2)
    mm1(2)
    r0(2)
    s4(3)
    mm2(2)
    s3(4)
    d0(1)
    s5(3)
    mm1(3)
    r0(3)
    r1(1)
    s4(4)
    mm2(3)
    s5(4)
    mm1(4)
    r0(4)
    mm2(4)
    hr_send()
    r1(2)
    d1()
    r2(0)
    r2(1)
    r1(3)
    r2(2)
    hr_wait()
    r1(4)
    d2()
    r2(3)
    r2(4)
    for d in sent:
        d.wait_send()


def exchange(ids, home, live, gates, lat, g, sv, w, xin):
    tok, d = g.shape
    pairs, hid = sv.shape
    kvr = lat.shape[1]
    frows = hid // 8
    drows = d // 128
    dma = pltpu.SemaphoreType.DMA
    v = pltpu.VMEM
    smem, vmem, hbm = (
        pl.BlockSpec(memory_space=m) for m in (pltpu.SMEM, pltpu.VMEM, pl.ANY)
    )
    ins = {
        "ids": vmem, "home": smem, "live": smem, "gates": vmem, "lat": vmem,
        "g": hbm, "sv": hbm, "w": hbm, "x": hbm,
    }
    outs = ("hg_out", "eg_out", "dg_out")
    scratch = {
        "hs": v((NXH, N_SLOT, tok, hid // NXH), BF),
        "hbuf": v((NX, NCORE, NZ, tok, hid // NXH), BF),
        "ht": v((hid // NXH, len(PLANE) * tok), BF),
        "wbuf": v((2, hid, max(WIDTHS)), BF),
        "acch": v((len(GROUP) * tok, hid), F32),
        "hret": v((NXL, NCORE, NZ, tok, hid), BF),
        "rbuf": v((N_SLOT, tok, hid), BF),
        "saved": v((pairs, hid), BF),
        "pick": v((N_SLOT, tok, pairs), BF),
        "pick_t": v((pairs, N_SLOT * tok), BF),
        "coef": v((N_SLOT, tok, 128), F32),
        "flip": v((2, 128, 128), F32),
        "xbuf": v((8, tok, d // 8), BF),
        "lsend": v((tok, kvr), BF),
        "lbuf": v((8, tok, kvr), BF),
        "dpart": v((d // 8, kvr), F32),
        "dsend": v((N_SLOT, drows, kvr), BF),
        "drecv": v((N_SLOT, drows, kvr), BF),
        "loc": dma((N_CHUNK + 3,)),
        "w_sem": dma((2,)),
    }
    for i, width in enumerate(WIDTHS):
        scratch["gbuf" + str(i)] = v((NX, NCORE, NZ, tok, width), BF)
        scratch["part" + str(i)] = v((NY - 1, frows, width), BF)
        scratch["relay" + str(i)] = v((2, frows // 2, width), BF)
        scratch["recv_p" + str(i)] = v((frows, width), BF)
        scratch["recv_m" + str(i)] = v((frows, width), BF)
    pairs_of = {
        "a1": (N_CHUNK, 6), "a2": (N_CHUNK, 4), "b1": (N_CHUNK, 4), "b2": (N_CHUNK, 4),
        "dd": (N_CHUNK, 8), "h": (32,), "rs": (N_CHUNK, 6), "hr": (16,), "dx": (8,),
        "dl": (8,), "ds": (16,),
    }
    for name, shape in pairs_of.items():
        scratch[name + "_s"] = dma(shape)
        scratch[name + "_r"] = dma(shape)
    names = tuple(ins) + outs + tuple(scratch)

    def body(*refs):
        kernel(names, *refs)

    return pl.pallas_call(
        body,
        out_shape=(
            v((pairs, hid), BF),
            v((frows, d), F32),
            v((drows, kvr), F32),
        ),
        in_specs=list(ins.values()),
        out_specs=(vmem, vmem, vmem),
        scratch_shapes=list(scratch.values()),
        compiler_params=pltpu.CompilerParams(
            collective_id=0, has_side_effects=True, vmem_limit_bytes=56 * 1024 * 1024
        ),
        name="exchange",
    )(ids, home, live, gates, lat, g, sv, w, xin)


def on_device(
    expert_ids,
    expert_home,
    live_tokens,
    gate_weights,
    output_grad,
    saved_hidden,
    down_weight,
    dense_input,
    latent_grad,
):
    tok, topk = expert_ids.shape
    hid = saved_hidden.shape[2]
    hg, eg, dg = exchange(
        expert_ids.T,
        expert_home,
        live_tokens,
        gate_weights.T,
        latent_grad,
        output_grad,
        saved_hidden.reshape(tok * topk, hid),
        down_weight[0],
        dense_input,
    )
    return hg.reshape(tok, topk, hid), eg[None], dg


def solution(mesh):
    torus = Mesh(mesh.devices.reshape(4, 2, 4, 2, 2), ALL)
    in_specs = (
        P(ALL, None),
        P(),
        P(ALL),
        P(ALL, None),
        P(ALL, None),
        P(ALL, None, None),
        P(EXPERT, None, None),
        P(ALL, None),
        P(ALL, None),
    )
    out_specs = (P(ALL, None, None), P(EXPERT, DP, None), P(ALL, None))
    return jax.shard_map(
        on_device, mesh=torus, in_specs=in_specs, out_specs=out_specs, check_vma=False
    )
```

```python
import jax
import jax.numpy as jnp
from jax import lax
from jax.experimental import pallas as pl
from jax.experimental.pallas import tpu as pltpu
from jax.sharding import Mesh
from jax.sharding import PartitionSpec as P

DP = ("y", "xh")
EXPERT = ("z", "xl", "c")
ALL = ("y", "xh", "z", "xl", "c")
MESH = pl.DeviceIdType.MESH
NY, NX, NZ, NCORE, NXH, NXL = 4, 4, 4, 2, 2, 2
N_SLOT = 16
BF = jnp.bfloat16
F32 = jnp.float32
WIDTHS = (1024, 1536, 2048, 1536, 1024)
N_CHUNK = len(WIDTHS)
STARTS = tuple(sum(WIDTHS[:i]) for i in range(N_CHUNK))
PLANE = [(i, j, k) for i in range(NX) for j in range(NCORE) for k in range(NZ)]
GROUP = [(i, j, k) for i in range(NXL) for j in range(NCORE) for k in range(NZ)]
ORDER = (2, 1, 3, 0)
PARTS = ((0, 1), (1, 3), (3, 4))


def up(v, k, n):
    return lax.rem(v + k, n)


def kernel(names, *all_refs):
    r = dict(zip(names, all_refs))
    ids, home, live, gates, lat = (r[k] for k in ("ids", "home", "live", "gates", "lat"))
    g_hbm, sv_hbm, w_hbm, x_hbm = (r[k] for k in ("g", "sv", "w", "x"))
    hg_out, eg_out, dg_out = r["hg_out"], r["eg_out"], r["dg_out"]
    gbuf, part, relay, recv_p, recv_m = (
        [r[k + str(i)] for i in range(N_CHUNK)] for k in ("gbuf", "part", "relay", "recv_p", "recv_m")
    )
    hs, hbuf, ht, wbuf, acch, hret, rbuf = (
        r[k] for k in ("hs", "hbuf", "ht", "wbuf", "acch", "hret", "rbuf")
    )
    saved, pick, pick_t, coef, flip = (r[k] for k in ("saved", "pick", "pick_t", "coef", "flip"))
    xbuf, xfwd, lsend, lbuf, dpart, dsend, drecv = (
        r[k] for k in ("xbuf", "xfwd", "lsend", "lbuf", "dpart", "dsend", "drecv")
    )

    y = lax.axis_index("y")
    xh = lax.axis_index("xh")
    z = lax.axis_index("z")
    xl = lax.axis_index("xl")
    c = lax.axis_index("c")
    x = xh * NXL + xl
    slot = z * 4 + xl * 2 + c
    tok = g_hbm.shape[0]
    half_tok = tok // 2
    topk = ids.shape[0]
    pairs = tok * topk
    frows = ht.shape[0] // NY
    hrow = frows // 2
    hid = w_hbm.shape[0]
    dcols = xbuf.shape[-1]
    drows = drecv.shape[1]
    rows_of = (pl.ds(0, half_tok), pl.ds(half_tok, half_tok))

    def at_x(v):
        return {"xh": v // NXL, "xl": lax.rem(v, NXL)}

    xp, xm, x2 = up(x, 1, NX), up(x, NX - 1, NX), up(x, 2, NX)
    zp, zm, z2 = up(z, 1, NZ), up(z, NZ - 1, NZ), up(z, 2, NZ)
    yp, ym = up(y, 1, NY), up(y, NY - 1, NY)
    dev_x = (at_x(xp), at_x(xm), at_x(x2))
    dev_z = ({"z": zp}, {"z": zm}, {"z": z2})
    dev_y = ({"y": yp}, {"y": ym})
    sibling = {"c": 1 - c}
    classes = {}

    def sems(name, at, out):
        return r["out"].at[classes.setdefault(out, len(classes))], r[name].at[at]

    def remote(src, dst, pair, dev):
        return pltpu.make_async_remote_copy(
            src_ref=src,
            dst_ref=dst,
            send_sem=pair[0],
            recv_sem=pair[1],
            device_id=dev,
            device_id_type=MESH,
        )

    def send(src, dst, pair, dev):
        remote(src, dst, pair, dev).start()

    def arrived(ref, name, at):
        sem = r[name].at[at]
        remote(ref, ref, (sem, sem), sibling).wait_recv()

    def gone(ref, out):
        sem = r["out"].at[classes[out]]
        remote(ref, ref, (sem, sem), sibling).wait_send()

    def plane_dev(n):
        i, j, k = PLANE[n]
        tx, tc, tz = up(x, i, NX), up(c, j, NCORE), up(z, k, NZ)
        return tx, tc, tz, {"xh": tx // NXL, "xl": lax.rem(tx, NXL), "z": tz, "c": tc}

    barrier = pltpu.get_barrier_semaphore()

    def greet():
        for n in range(1, len(PLANE)):
            pl.semaphore_signal(barrier, inc=1, device_id=plane_dev(n)[3], device_id_type=MESH)
        for i in range(1, NY):
            pl.semaphore_signal(barrier, inc=1, device_id={"y": up(y, i, NY)}, device_id_type=MESH)

    def bar():
        pl.semaphore_wait(barrier, len(PLANE) - 1 + NY - 1)

    def own_copy(ch):
        return pltpu.make_async_copy(
            g_hbm.at[:, pl.ds(STARTS[ch], WIDTHS[ch])], gbuf[ch].at[x, c, z], r["loc"].at[0]
        )

    def saved_copy():
        return pltpu.make_async_copy(sv_hbm, saved, r["loc"].at[1])

    def h_local(which):
        lo, hi = PARTS[which]
        col = pl.ds(lo * frows, (hi - lo) * frows)
        return pltpu.make_async_copy(
            hs.at[xh, slot, :, col], hbuf.at[x, c, z, :, col], r["h"].at[which]
        )

    def x_cols(ty, th):
        return x_hbm.at[:, pl.ds(pl.multiple_of((ty * 2 + th) * dcols, 128), dcols)]

    def d_local():
        return pltpu.make_async_copy(x_cols(y, xh), xbuf.at[y, xh], r["dx"].at[0])

    def f_local():
        return pltpu.make_async_copy(x_cols(y, 1 - xh), xfwd.at[y], r["dx"].at[1])

    def w_copy(ch):
        return pltpu.make_async_copy(
            w_hbm.at[:, pl.ds(STARTS[ch], WIDTHS[ch])],
            wbuf.at[ch % 2, :, pl.ds(0, WIDTHS[ch])],
            r["w_sem"].at[ch % 2],
        )

    def prep():
        homes = jnp.zeros(ids.shape, F32)
        for e in range(N_SLOT):
            homes = jnp.where(ids[...] == e, home[e].astype(F32), homes)
        is_live = lax.broadcasted_iota(jnp.int32, ids.shape, 1) < live[0]
        flip[...] = jnp.zeros_like(flip)
        flip[0, 0:topk, 0:tok] = homes
        flip[1, 0:topk, 0:tok] = jnp.where(is_live, gates[...], jnp.zeros_like(gates))
        home_t = flip[0].T[0:tok]
        scale_t = flip[1].T[0:tok]
        lane = lax.broadcasted_iota(jnp.int32, (128, pairs), 1)
        row = lax.broadcasted_iota(jnp.int32, (128, pairs), 0)
        spread = jnp.where(lax.rem(lane, topk) == row, 1.0, 0.0).astype(BF)
        wide = jnp.dot(home_t.astype(BF), spread, preferred_element_type=F32)
        lane = lax.broadcasted_iota(jnp.int32, (tok, pairs), 1)
        row = lax.broadcasted_iota(jnp.int32, (tok, pairs), 0)
        wide = jnp.where(lane // topk == row, wide, -1.0)
        column = lax.broadcasted_iota(jnp.int32, (tok, 128), 1)
        for s in range(N_SLOT):
            pick[s] = jnp.where(wide == float(s), 1.0, 0.0).astype(BF)
            mine = jnp.where((home_t == float(s)) & (column < topk), scale_t, 0.0)
            coef[s] = jnp.broadcast_to(jnp.sum(mine, axis=1, keepdims=True), (tok, 128))
        token = lax.broadcasted_iota(jnp.int32, lat.shape, 0)
        lsend[...] = jnp.where(token < live[0], lat[...], jnp.zeros_like(lat))
        saved_copy().wait()
        table = pick[...].reshape(N_SLOT * tok, pairs)
        scale = coef[...].reshape(N_SLOT * tok, 128)
        for n, k in enumerate(ORDER):
            col = pl.ds(pl.multiple_of(up(y, k, NY) * NXH * frows, NXH * frows), NXH * frows)
            rows = jnp.dot(table, saved[:, col], preferred_element_type=F32)
            for j in range(NXH):
                scaled = (rows[:, j * frows : (j + 1) * frows] * scale).astype(BF)
                hs[j, :, :, n * frows : (n + 1) * frows] = scaled.reshape(N_SLOT, tok, frows)

    def lanes(ch, h):
        return pl.ds(h * (WIDTHS[ch] // 2), WIDTHS[ch] // 2)

    def direct(ch):
        return ch == 0

    def own_wait():
        pltpu.make_async_copy(g_hbm, g_hbm, r["loc"].at[0]).wait()

    def s0(ch):
        for h in range(2):
            ref = gbuf[ch].at[x, c, z, :, lanes(ch, h)]
            for s in range(3 if direct(ch) else 2):
                at = 0 if direct(ch) else ch * 4 + h * 2 + s
                send(ref, ref, sems("a1", at, ("a", ch)), (dev_x, dev_z)[h][s])

    def s1(ch):
        for h in range(2):
            for s in range(2):
                if h == 0:
                    blk = gbuf[ch].at[(xm, xp)[s], c, z]
                else:
                    blk = gbuf[ch].at[x, c, (zm, zp)[s]]
                dev = (dev_x, dev_z)[h][s]
                arrived(blk.at[:, lanes(ch, h)], "a1", ch * 4 + h * 2 + s)
                ref = blk.at[rows_of[s], lanes(ch, h)]
                send(ref, ref, sems("a2", ch, ("a", ch)), dev)

    def line(ch, h, other):
        if h == 0:
            return gbuf[ch].at[:, c, other, :, lanes(ch, 0)]
        return gbuf[ch].at[other, c, :, :, lanes(ch, 1)]

    def line_half(ch, h, other, s):
        if h == 0:
            return gbuf[ch].at[:, c, other, rows_of[s], lanes(ch, 0)]
        return gbuf[ch].at[other, c, :, rows_of[s], lanes(ch, 1)]

    def s2(ch):
        if direct(ch):
            arrived(gbuf[ch].at[0:3, c, z], "a1", 0)
        else:
            arrived(gbuf[ch].at[0, c, z], "a2", ch)
        for h in range(2):
            ref = line(ch, h, (z, x)[h])
            for s in range(2):
                send(ref, ref, sems("b1", ch * 4 + h * 2 + s, ("b", ch)), (dev_z, dev_x)[h][s])
            send(ref, ref, sems("dd", ch, ("d", ch)), sibling)

    def s3(ch):
        for h in range(2):
            for s in range(2):
                other = ((zm, zp), (xm, xp))[h][s]
                dev = (dev_z, dev_x)[h][s]
                ref = line(ch, h, other)
                arrived(ref, "b1", ch * 4 + h * 2 + s)
                fwd = line_half(ch, h, other, s)
                send(fwd, fwd, sems("b2", ch, ("b", ch)), dev)
                send(ref, ref, sems("dd", ch, ("d", ch)), sibling)

    def s4(ch):
        arrived(gbuf[ch].at[:, c, z], "b2", ch)
        for h in range(2):
            ref = line(ch, h, (z2, x2)[h])
            send(ref, ref, sems("dd", ch, ("d", ch)), sibling)

    def s5(ch):
        arrived(gbuf[ch].at[:, 1 - c], "dd", ch)

    def h_send(first, last, which):
        if first == 0:
            h_local(which).start()
        lo, hi = PARTS[which]
        col = pl.ds(lo * frows, (hi - lo) * frows)
        for m in range(first, last):
            n = ((m + 1) * 11) % len(PLANE)
            tx, tc, tz, dev = plane_dev(n)
            t_slot = tz * 4 + lax.rem(tx, NXL) * 2 + tc
            src = hs.at[tx // NXL, t_slot, :, col]
            send(src, hbuf.at[x, c, z, :, col], sems("h", which, "h"), dev)

    def h_build(which):
        lo, hi = PARTS[which]
        col = pl.ds(lo * frows, (hi - lo) * frows)
        arrived(hbuf.at[:, :, :, :, col], "h", which)
        n_tok = NCORE * NZ * tok
        for k in range(lo, hi):
            for i in range(NX):
                blk = hbuf[i, :, :, :, k * frows : (k + 1) * frows].reshape(n_tok, frows)
                ht[pl.ds(k * frows, frows), pl.ds(i * n_tok, n_tok)] = blk.T

    def mm1(ch, lo=0, hi=NY):
        def body(n, carry):
            col = pl.ds(pl.multiple_of(n * 256, 256), 256)
            g = gbuf[ch][:, :, :, :, col].reshape(len(PLANE) * tok, 256)
            p = jnp.dot(ht[lo * frows : hi * frows], g, preferred_element_type=F32)
            for k in range(lo, hi):
                rows = p[(k - lo) * frows : (k - lo + 1) * frows]
                if k == NY - 1:
                    eg_out[:, pl.ds(pl.multiple_of(STARTS[ch] + n * 256, 256), 256)] = rows
                else:
                    part[ch][k, :, col] = rows.astype(BF)
            return carry

        lax.fori_loop(0, WIDTHS[ch] // 256, body, 0)

    def m0(which):
        mm1(0, *PARTS[which])

    def mm2(ch):
        w_copy(ch).wait()

        def body(n, carry):
            row = pl.ds(pl.multiple_of(n * 256, 256), 256)
            g = gbuf[ch][pl.ds(xh * NXL, NXL)].reshape(len(GROUP) * tok, WIDTHS[ch])
            w = wbuf[ch % 2, row, pl.ds(0, WIDTHS[ch])]
            p = lax.dot_general(g, w, (((1,), (1,)), ((), ())), preferred_element_type=F32)
            if ch == 0:
                acch[:, row] = p
            else:
                acch[:, row] = acch[:, row] + p
            return carry

        lax.fori_loop(0, hid // 256, body, 0)
        if ch + 2 < N_CHUNK:
            w_copy(ch + 2).start()

    row_a, row_b = pl.ds(0, hrow), pl.ds(hrow, hrow)

    def r0a(ch):
        p = part[ch]
        send(p.at[0, row_b], relay[ch].at[0], sems("rs", ch * 3 + 0, ("r", ch)), dev_y[0])
        send(p.at[0, row_a], relay[ch].at[1], sems("rs", ch * 3 + 1, ("r", ch)), dev_y[1])

    def r0b(ch):
        p = part[ch]
        send(p.at[1, row_a], recv_m[ch].at[row_a], sems("rs", ch * 3 + 2, ("r", ch)), dev_y[0])
        send(p.at[2, row_b], recv_p[ch].at[row_b], sems("rs", ch * 3 + 2, ("r", ch)), dev_y[1])

    def r1(ch):
        p = part[ch]
        arrived(relay[ch].at[0], "rs", ch * 3)
        p[1, row_b] = (p[1, row_b].astype(F32) + relay[ch][0].astype(F32)).astype(BF)
        send(p.at[1, row_b], recv_m[ch].at[row_b], sems("rs", ch * 3 + 2, ("r", ch)), dev_y[0])
        arrived(relay[ch].at[1], "rs", ch * 3 + 1)
        p[2, row_a] = (p[2, row_a].astype(F32) + relay[ch][1].astype(F32)).astype(BF)
        send(p.at[2, row_a], recv_p[ch].at[row_a], sems("rs", ch * 3 + 2, ("r", ch)), dev_y[1])

    def r2(ch):
        arrived(part[ch].at[0:2], "rs", ch * 3 + 2)
        col = pl.ds(STARTS[ch], WIDTHS[ch])
        eg_out[:, col] = eg_out[:, col] + (recv_m[ch][...].astype(F32) + recv_p[ch][...].astype(F32))

    def group_dev(n):
        i, j, k = GROUP[n]
        tx, tc, tz = up(xl, i, NXL), up(c, j, NCORE), up(z, k, NZ)
        return tx, tc, tz, {"xl": tx, "z": tz, "c": tc}

    def hr_send():
        hret[...] = acch[...].astype(BF).reshape(hret.shape)
        for n in range(1, len(GROUP)):
            tx, tc, tz, dev = group_dev(n)
            send(hret.at[tx, tc, tz], rbuf.at[slot], sems("hr", 0, "hr"), dev)
        pltpu.make_async_copy(hret.at[xl, c, z], rbuf.at[slot], r["hr"].at[0]).start()

    def table_flip():
        pick_t[...] = pick[...].reshape(N_SLOT * tok, pairs).T

    def hr_wait():
        arrived(rbuf, "hr", 0)
        scale = coef[...].reshape(N_SLOT * tok, 128)
        for n in range(hid // 256):
            halves = []
            for j in range(2):
                rows = rbuf[:, :, n * 256 + j * 128 : n * 256 + (j + 1) * 128]
                rows = rows.reshape(N_SLOT * tok, 128).astype(F32) * scale
                halves.append(rows.astype(BF))
            rows = jnp.concatenate(halves, axis=1)
            back = jnp.dot(pick_t[...], rows, preferred_element_type=F32)
            hg_out[:, n * 256 : (n + 1) * 256] = back.astype(BF)

    def d0a():
        d_local().start()
        f_local().start()
        lbuf[y, xh] = lsend[...]
        for i in range(1, NY):
            ty = up(y, i, NY)
            dev = {"y": ty}
            send(x_cols(ty, 1 - xh), xfwd.at[y], sems("dx", 1, "dx"), dev)
            send(lsend, lbuf.at[y, xh], sems("dl", 0, "dl"), dev)
            send(x_cols(ty, xh), xbuf.at[y, xh], sems("dx", 0, "dx"), dev)

    def d0b():
        arrived(xfwd, "dx", 1)
        arrived(lbuf.at[0:3, xh], "dl", 0)
        dev = {"xh": 1 - xh}
        send(xfwd, xbuf.at[:, xh], sems("dx", 0, "dxf"), dev)
        send(lbuf.at[:, xh], lbuf.at[:, xh], sems("dl", 1, "dlf"), dev)

    def d1():
        arrived(xbuf, "dx", 0)
        arrived(lbuf.at[:, xh], "dl", 1)
        n_tok = NY * NXH * tok

        def body(n, carry):
            col = pl.ds(pl.multiple_of(n * 128, 128), 128)
            xt = xbuf[:, :, :, col].reshape(n_tok, 128).T
            dpart[col, :] = jnp.dot(
                xt, lbuf[...].reshape(n_tok, lbuf.shape[-1]), preferred_element_type=F32
            )
            return carry

        lax.fori_loop(0, dcols // 128, body, 0)
        for n in range(N_SLOT):
            dsend[n] = dpart[n * drows : (n + 1) * drows].astype(BF)
        for n in range(1, len(GROUP)):
            tx, tc, tz, dev = group_dev(n)
            send(dsend.at[tz * 4 + tx * 2 + tc], drecv.at[slot], sems("ds", 0, "ds"), dev)
        pltpu.make_async_copy(dsend.at[slot], drecv.at[slot], r["ds"].at[0]).start()

    def d2():
        arrived(drecv, "ds", 0)
        mine = dpart[pl.ds(pl.multiple_of(slot * drows, 8), drows)]
        total = mine - drecv[slot].astype(F32)
        for n in range(len(GROUP)):
            total = total + drecv[n].astype(F32)
        dg_out[...] = total

    def sendwait():
        for ch in range(N_CHUNK):
            gone(gbuf[ch].at[0:3, c, z], ("a", ch))
            gone(gbuf[ch].at[0:3, c], ("b", ch))
            gone(gbuf[ch].at[:, c], ("d", ch))
            gone(part[ch], ("r", ch))
        gone(ht.at[0 : ht.shape[0] // 32 * 31], "h")
        gone(wbuf.at[0, pl.ds(0, (len(GROUP) - 1) * tok), pl.ds(0, hid)], "hr")
        gone(dsend.at[0 : N_SLOT - 1], "ds")
        gone(xbuf.at[0:3], "dx")
        gone(xfwd, "dxf")
        gone(lbuf.at[0:3, xh], "dl")
        gone(lbuf.at[:, xh], "dlf")

    greet()
    saved_copy().start()
    own_copy(0).start()
    own_copy(1).start()
    own_copy(2).start()
    own_copy(3).start()
    own_copy(4).start()
    w_copy(0).start()
    w_copy(1).start()
    prep()
    own_wait()
    bar()
    h_send(24, 31, 0)
    h_send(8, 16, 1)
    h_send(0, 8, 1)
    s0(0)
    s0(1)
    h_send(16, 24, 0)
    h_send(24, 31, 1)
    s2(0)
    h_send(0, 8, 0)
    h_send(16, 24, 1)
    s1(1)
    d0a()
    s3(0)
    h_send(8, 16, 0)
    table_flip()
    s0(3)
    s0(2)
    h_send(16, 24, 2)
    h_build(1)
    s2(1)
    h_send(24, 31, 2)
    s4(0)
    s1(2)
    s5(0)
    h_send(0, 8, 2)
    h_build(0)
    m0(0)
    r0a(0)
    h_send(8, 16, 2)
    s3(1)
    m0(1)
    s2(2)
    r0b(0)
    r1(0)
    mm2(0)
    s0(4)
    s1(3)
    h_build(2)
    s4(1)
    m0(2)
    s5(1)
    mm1(1)
    r0a(1)
    r0b(1)
    s3(2)
    mm2(1)
    s1(4)
    s2(3)
    s4(2)
    s2(4)
    s5(2)
    r1(1)
    mm1(2)
    s3(3)
    r0b(2)
    r0a(2)
    r2(0)
    s3(4)
    mm2(2)
    s4(3)
    s4(4)
    d0b()
    s5(3)
    mm1(3)
    s5(4)
    r0a(3)
    mm2(3)
    r0b(3)
    mm2(4)
    hr_send()
    d1()
    r1(2)
    r2(1)
    mm1(4)
    r0b(4)
    r0a(4)
    r1(3)
    r2(2)
    r1(4)
    r2(3)
    d2()
    hr_wait()
    r2(4)
    sendwait()


def exchange(ids, home, live, gates, lat, g, sv, w, xin):
    tok, d = g.shape
    pairs, hid = sv.shape
    kvr = lat.shape[1]
    frows = hid // 8
    drows = d // 128
    dma = pltpu.SemaphoreType.DMA
    v = pltpu.VMEM
    smem, vmem, hbm = (
        pl.BlockSpec(memory_space=m) for m in (pltpu.SMEM, pltpu.VMEM, pl.ANY)
    )
    ins = {
        "ids": vmem, "home": smem, "live": smem, "gates": vmem, "lat": vmem,
        "g": hbm, "sv": hbm, "w": hbm, "x": hbm,
    }
    outs = ("hg_out", "eg_out", "dg_out")
    scratch = {
        "hs": v((NXH, N_SLOT, tok, hid // NXH), BF),
        "hbuf": v((NX, NCORE, NZ, tok, hid // NXH), BF),
        "ht": v((hid // NXH, len(PLANE) * tok), BF),
        "wbuf": v((2, hid, max(WIDTHS)), BF),
        "acch": v((len(GROUP) * tok, hid), F32),
        "hret": v((NXL, NCORE, NZ, tok, hid), BF),
        "rbuf": v((N_SLOT, tok, hid), BF),
        "saved": v((pairs, hid), BF),
        "pick": v((N_SLOT, tok, pairs), BF),
        "pick_t": v((pairs, N_SLOT * tok), BF),
        "coef": v((N_SLOT, tok, 128), F32),
        "flip": v((2, 128, 128), F32),
        "xbuf": v((NY, NXH, tok, d // 8), BF),
        "xfwd": v((NY, tok, d // 8), BF),
        "lsend": v((tok, kvr), BF),
        "lbuf": v((NY, NXH, tok, kvr), BF),
        "dpart": v((d // 8, kvr), F32),
        "dsend": v((N_SLOT, drows, kvr), BF),
        "drecv": v((N_SLOT, drows, kvr), BF),
    }
    for i, width in enumerate(WIDTHS):
        scratch["gbuf" + str(i)] = v((NX, NCORE, NZ, tok, width), BF)
        scratch["part" + str(i)] = v((NY - 1, frows, width), BF)
        scratch["relay" + str(i)] = v((2, frows // 2, width), BF)
        scratch["recv_p" + str(i)] = v((frows, width), BF)
        scratch["recv_m" + str(i)] = v((frows, width), BF)
    counts = {
        "a1": N_CHUNK * 4, "a2": N_CHUNK, "b1": N_CHUNK * 4, "b2": N_CHUNK, "dd": N_CHUNK,
        "h": len(PARTS), "rs": N_CHUNK * 3, "hr": 1, "dx": 2, "dl": 2, "ds": 1,
        "loc": 2, "w_sem": 2, "out": N_CHUNK * 4 + 7,
    }
    for name, count in counts.items():
        scratch[name] = dma((count,))
    names = tuple(ins) + outs + tuple(scratch)

    def body(*refs):
        kernel(names, *refs)

    return pl.pallas_call(
        body,
        out_shape=(
            v((pairs, hid), BF),
            v((frows, d), F32),
            v((drows, kvr), F32),
        ),
        in_specs=list(ins.values()),
        out_specs=(vmem, vmem, vmem),
        scratch_shapes=list(scratch.values()),
        compiler_params=pltpu.CompilerParams(
            collective_id=0, has_side_effects=True, vmem_limit_bytes=56 * 1024 * 1024
        ),
        name="exchange",
    )(ids, home, live, gates, lat, g, sv, w, xin)


def on_device(
    expert_ids,
    expert_home,
    live_tokens,
    gate_weights,
    output_grad,
    saved_hidden,
    down_weight,
    dense_input,
    latent_grad,
):
    tok, topk = expert_ids.shape
    hid = saved_hidden.shape[2]
    hg, eg, dg = exchange(
        expert_ids.T,
        expert_home,
        live_tokens,
        gate_weights.T,
        latent_grad,
        output_grad,
        saved_hidden.reshape(tok * topk, hid),
        down_weight[0],
        dense_input,
    )
    return hg.reshape(tok, topk, hid), eg[None], dg


def solution(mesh):
    torus = Mesh(mesh.devices.reshape(4, 2, 4, 2, 2), ALL)
    in_specs = (
        P(ALL, None),
        P(),
        P(ALL),
        P(ALL, None),
        P(ALL, None),
        P(ALL, None, None),
        P(EXPERT, None, None),
        P(ALL, None),
        P(ALL, None),
    )
    out_specs = (P(ALL, None, None), P(EXPERT, DP, None), P(ALL, None))
    return jax.shard_map(
        on_device, mesh=torus, in_specs=in_specs, out_specs=out_specs, check_vma=False
    )
```

```python
import jax
import jax.numpy as jnp
from jax import lax
from jax.experimental import pallas as pl
from jax.experimental.pallas import tpu as pltpu
from jax.sharding import Mesh
from jax.sharding import PartitionSpec as P

DP = ("y", "xh")
EXPERT = ("z", "xl", "c")
ALL = ("y", "xh", "z", "xl", "c")
MESH = pl.DeviceIdType.MESH
NY, NX, NZ, NCORE, NXH, NXL = 4, 4, 4, 2, 2, 2
N_SLOT = 16
BF = jnp.bfloat16
F32 = jnp.float32
WIDTHS = (1024, 1536, 2048, 1536, 1024)
N_CHUNK = len(WIDTHS)
STARTS = tuple(sum(WIDTHS[:i]) for i in range(N_CHUNK))
PLANE = [(i, j, k) for i in range(NX) for j in range(NCORE) for k in range(NZ)]
GROUP = [(i, j, k) for i in range(NXL) for j in range(NCORE) for k in range(NZ)]
ORDER = (2, 1, 3, 0)
PARTS = ((0, 1), (1, 3), (3, 4))


def up(v, k, n):
    return lax.rem(v + k, n)


def kernel(names, *all_refs):
    r = dict(zip(names, all_refs))
    ids, home, live, gates, lat = (r[k] for k in ("ids", "home", "live", "gates", "lat"))
    g_hbm, sv_hbm, w_hbm, x_hbm = (r[k] for k in ("g", "sv", "w", "x"))
    hg_out, eg_out, dg_out = r["hg_out"], r["eg_out"], r["dg_out"]
    gbuf, part, relay, recv_p, recv_m = (
        [r[k + str(i)] for i in range(N_CHUNK)] for k in ("gbuf", "part", "relay", "recv_p", "recv_m")
    )
    hs, hbuf, ht, wbuf, acch, hret, rbuf = (
        r[k] for k in ("hs", "hbuf", "ht", "wbuf", "acch", "hret", "rbuf")
    )
    saved, pick, pick_t, coef, flip = (r[k] for k in ("saved", "pick", "pick_t", "coef", "flip"))
    xbuf, xfwd, xrel, lsend, lbuf, dpart, dsend, drecv = (
        r[k] for k in ("xbuf", "xfwd", "xrel", "lsend", "lbuf", "dpart", "dsend", "drecv")
    )

    y = lax.axis_index("y")
    xh = lax.axis_index("xh")
    z = lax.axis_index("z")
    xl = lax.axis_index("xl")
    c = lax.axis_index("c")
    x = xh * NXL + xl
    slot = z * 4 + xl * 2 + c
    tok = g_hbm.shape[0]
    half_tok = tok // 2
    topk = ids.shape[0]
    pairs = tok * topk
    frows = ht.shape[0] // NY
    hrow = frows // 2
    hid = w_hbm.shape[0]
    dcols = xbuf.shape[-1]
    drows = drecv.shape[1]
    rows_of = (pl.ds(0, half_tok), pl.ds(half_tok, half_tok))

    def at_x(v):
        return {"xh": v // NXL, "xl": lax.rem(v, NXL)}

    xp, xm, x2 = up(x, 1, NX), up(x, NX - 1, NX), up(x, 2, NX)
    zp, zm, z2 = up(z, 1, NZ), up(z, NZ - 1, NZ), up(z, 2, NZ)
    yp, ym = up(y, 1, NY), up(y, NY - 1, NY)
    dev_x = (at_x(xp), at_x(xm), at_x(x2))
    dev_z = ({"z": zp}, {"z": zm}, {"z": z2})
    dev_y = ({"y": yp}, {"y": ym})
    sibling = {"c": 1 - c}
    classes = {}

    def sems(name, at, out):
        return r["out"].at[classes.setdefault(out, len(classes))], r[name].at[at]

    def remote(src, dst, pair, dev):
        return pltpu.make_async_remote_copy(
            src_ref=src,
            dst_ref=dst,
            send_sem=pair[0],
            recv_sem=pair[1],
            device_id=dev,
            device_id_type=MESH,
        )

    def send(src, dst, pair, dev):
        remote(src, dst, pair, dev).start()

    def arrived(ref, name, at):
        sem = r[name].at[at]
        remote(ref, ref, (sem, sem), sibling).wait_recv()

    def gone(ref, out):
        sem = r["out"].at[classes[out]]
        remote(ref, ref, (sem, sem), sibling).wait_send()

    def plane_dev(n):
        i, j, k = PLANE[n]
        tx, tc, tz = up(x, i, NX), up(c, j, NCORE), up(z, k, NZ)
        return tx, tc, tz, {"xh": tx // NXL, "xl": lax.rem(tx, NXL), "z": tz, "c": tc}

    barrier = pltpu.get_barrier_semaphore()

    def greet():
        for n in range(1, len(PLANE)):
            pl.semaphore_signal(barrier, inc=1, device_id=plane_dev(n)[3], device_id_type=MESH)
        for i in range(1, NY):
            pl.semaphore_signal(barrier, inc=1, device_id={"y": up(y, i, NY)}, device_id_type=MESH)

    def bar():
        pl.semaphore_wait(barrier, len(PLANE) - 1 + NY - 1)

    def own_copy(ch):
        return pltpu.make_async_copy(
            g_hbm.at[:, pl.ds(STARTS[ch], WIDTHS[ch])], gbuf[ch].at[x, c, z], r["loc"].at[0]
        )

    def saved_copy():
        return pltpu.make_async_copy(sv_hbm, saved, r["loc"].at[1])

    def h_local(which):
        lo, hi = PARTS[which]
        col = pl.ds(lo * frows, (hi - lo) * frows)
        return pltpu.make_async_copy(
            hs.at[xh, slot, :, col], hbuf.at[x, c, z, :, col], r["h"].at[which]
        )

    def x_cols(ty, th):
        return x_hbm.at[:, pl.ds(pl.multiple_of((ty * 2 + th) * dcols, 128), dcols)]

    def d_local():
        return pltpu.make_async_copy(x_cols(y, xh), xbuf.at[y, xh], r["dx"].at[0])

    def f_local():
        return pltpu.make_async_copy(x_cols(y, 1 - xh), xfwd.at[y], r["dx"].at[1])

    def w_copy(ch):
        return pltpu.make_async_copy(
            w_hbm.at[:, pl.ds(STARTS[ch], WIDTHS[ch])],
            wbuf.at[ch % 2, :, pl.ds(0, WIDTHS[ch])],
            r["w_sem"].at[ch % 2],
        )

    def prep():
        homes = jnp.zeros(ids.shape, F32)
        for e in range(N_SLOT):
            homes = jnp.where(ids[...] == e, home[e].astype(F32), homes)
        is_live = lax.broadcasted_iota(jnp.int32, ids.shape, 1) < live[0]
        flip[...] = jnp.zeros_like(flip)
        flip[0, 0:topk, 0:tok] = homes
        flip[1, 0:topk, 0:tok] = jnp.where(is_live, gates[...], jnp.zeros_like(gates))
        home_t = flip[0].T[0:tok]
        scale_t = flip[1].T[0:tok]
        lane = lax.broadcasted_iota(jnp.int32, (128, pairs), 1)
        row = lax.broadcasted_iota(jnp.int32, (128, pairs), 0)
        spread = jnp.where(lax.rem(lane, topk) == row, 1.0, 0.0).astype(BF)
        wide = jnp.dot(home_t.astype(BF), spread, preferred_element_type=F32)
        lane = lax.broadcasted_iota(jnp.int32, (tok, pairs), 1)
        row = lax.broadcasted_iota(jnp.int32, (tok, pairs), 0)
        wide = jnp.where(lane // topk == row, wide, -1.0)
        column = lax.broadcasted_iota(jnp.int32, (tok, 128), 1)
        for s in range(N_SLOT):
            pick[s] = jnp.where(wide == float(s), 1.0, 0.0).astype(BF)
            mine = jnp.where((home_t == float(s)) & (column < topk), scale_t, 0.0)
            coef[s] = jnp.broadcast_to(jnp.sum(mine, axis=1, keepdims=True), (tok, 128))
        token = lax.broadcasted_iota(jnp.int32, lat.shape, 0)
        lsend[...] = jnp.where(token < live[0], lat[...], jnp.zeros_like(lat))
        saved_copy().wait()
        table = pick[...].reshape(N_SLOT * tok, pairs)
        scale = coef[...].reshape(N_SLOT * tok, 128)
        for n, k in enumerate(ORDER):
            col = pl.ds(pl.multiple_of(up(y, k, NY) * NXH * frows, NXH * frows), NXH * frows)
            rows = jnp.dot(table, saved[:, col], preferred_element_type=F32)
            for j in range(NXH):
                scaled = (rows[:, j * frows : (j + 1) * frows] * scale).astype(BF)
                hs[j, :, :, n * frows : (n + 1) * frows] = scaled.reshape(N_SLOT, tok, frows)

    def lanes(ch, h):
        return pl.ds(h * (WIDTHS[ch] // 2), WIDTHS[ch] // 2)

    def direct(ch):
        return ch == 0

    def own_wait():
        pltpu.make_async_copy(g_hbm, g_hbm, r["loc"].at[0]).wait()

    def s0(ch):
        for h in range(2):
            ref = gbuf[ch].at[x, c, z, :, lanes(ch, h)]
            for s in range(3 if direct(ch) else 2):
                at = 0 if direct(ch) else ch * 4 + h * 2 + s
                send(ref, ref, sems("a1", at, ("a", ch)), (dev_x, dev_z)[h][s])

    def s1(ch):
        for h in range(2):
            for s in range(2):
                if h == 0:
                    blk = gbuf[ch].at[(xm, xp)[s], c, z]
                else:
                    blk = gbuf[ch].at[x, c, (zm, zp)[s]]
                dev = (dev_x, dev_z)[h][s]
                arrived(blk.at[:, lanes(ch, h)], "a1", ch * 4 + h * 2 + s)
                ref = blk.at[rows_of[s], lanes(ch, h)]
                send(ref, ref, sems("a2", ch, ("a", ch)), dev)

    def line(ch, h, other):
        if h == 0:
            return gbuf[ch].at[:, c, other, :, lanes(ch, 0)]
        return gbuf[ch].at[other, c, :, :, lanes(ch, 1)]

    def line_half(ch, h, other, s):
        if h == 0:
            return gbuf[ch].at[:, c, other, rows_of[s], lanes(ch, 0)]
        return gbuf[ch].at[other, c, :, rows_of[s], lanes(ch, 1)]

    def s2(ch):
        if direct(ch):
            arrived(gbuf[ch].at[0:3, c, z], "a1", 0)
        else:
            arrived(gbuf[ch].at[0, c, z], "a2", ch)
        for h in range(2):
            ref = line(ch, h, (z, x)[h])
            for s in range(2):
                send(ref, ref, sems("b1", ch * 4 + h * 2 + s, ("b", ch)), (dev_z, dev_x)[h][s])
            send(ref, ref, sems("dd", ch, ("d", ch)), sibling)

    def s3(ch):
        for h in range(2):
            for s in range(2):
                other = ((zm, zp), (xm, xp))[h][s]
                dev = (dev_z, dev_x)[h][s]
                ref = line(ch, h, other)
                arrived(ref, "b1", ch * 4 + h * 2 + s)
                fwd = line_half(ch, h, other, s)
                send(fwd, fwd, sems("b2", ch, ("b", ch)), dev)
                send(ref, ref, sems("dd", ch, ("d", ch)), sibling)

    def s4(ch):
        arrived(gbuf[ch].at[:, c, z], "b2", ch)
        for h in range(2):
            ref = line(ch, h, (z2, x2)[h])
            send(ref, ref, sems("dd", ch, ("d", ch)), sibling)

    def s5(ch):
        arrived(gbuf[ch].at[:, 1 - c], "dd", ch)

    def h_send(first, last, which):
        if first == 0:
            h_local(which).start()
        lo, hi = PARTS[which]
        col = pl.ds(lo * frows, (hi - lo) * frows)
        for m in range(first, last):
            n = ((m + 1) * 11) % len(PLANE)
            tx, tc, tz, dev = plane_dev(n)
            t_slot = tz * 4 + lax.rem(tx, NXL) * 2 + tc
            src = hs.at[tx // NXL, t_slot, :, col]
            send(src, hbuf.at[x, c, z, :, col], sems("h", which, "h"), dev)

    def h_build(which):
        lo, hi = PARTS[which]
        col = pl.ds(lo * frows, (hi - lo) * frows)
        arrived(hbuf.at[:, :, :, :, col], "h", which)
        n_tok = NCORE * NZ * tok
        for k in range(lo, hi):
            for i in range(NX):
                blk = hbuf[i, :, :, :, k * frows : (k + 1) * frows].reshape(n_tok, frows)
                ht[pl.ds(k * frows, frows), pl.ds(i * n_tok, n_tok)] = blk.T

    def mm1(ch, lo=0, hi=NY):
        def body(n, carry):
            col = pl.ds(pl.multiple_of(n * 256, 256), 256)
            g = gbuf[ch][:, :, :, :, col].reshape(len(PLANE) * tok, 256)
            p = jnp.dot(ht[lo * frows : hi * frows], g, preferred_element_type=F32)
            for k in range(lo, hi):
                rows = p[(k - lo) * frows : (k - lo + 1) * frows]
                if k == NY - 1:
                    eg_out[:, pl.ds(pl.multiple_of(STARTS[ch] + n * 256, 256), 256)] = rows
                else:
                    part[ch][k, :, col] = rows.astype(BF)
            return carry

        lax.fori_loop(0, WIDTHS[ch] // 256, body, 0)

    def m0(which):
        mm1(0, *PARTS[which])

    def mm2(ch):
        w_copy(ch).wait()

        def body(n, carry):
            row = pl.ds(pl.multiple_of(n * 256, 256), 256)
            g = gbuf[ch][pl.ds(xh * NXL, NXL)].reshape(len(GROUP) * tok, WIDTHS[ch])
            w = wbuf[ch % 2, row, pl.ds(0, WIDTHS[ch])]
            p = lax.dot_general(g, w, (((1,), (1,)), ((), ())), preferred_element_type=F32)
            if ch == 0:
                acch[:, row] = p
            else:
                acch[:, row] = acch[:, row] + p
            return carry

        lax.fori_loop(0, hid // 256, body, 0)
        if ch + 2 < N_CHUNK:
            w_copy(ch + 2).start()

    row_a, row_b = pl.ds(0, hrow), pl.ds(hrow, hrow)

    def r0a(ch):
        p = part[ch]
        send(p.at[0, row_b], relay[ch].at[0], sems("rs", ch * 3 + 0, ("r", ch)), dev_y[0])
        send(p.at[0, row_a], relay[ch].at[1], sems("rs", ch * 3 + 1, ("r", ch)), dev_y[1])

    def r0b(ch):
        p = part[ch]
        send(p.at[1, row_a], recv_m[ch].at[row_a], sems("rs", ch * 3 + 2, ("r", ch)), dev_y[0])
        send(p.at[2, row_b], recv_p[ch].at[row_b], sems("rs", ch * 3 + 2, ("r", ch)), dev_y[1])

    def r1(ch):
        p = part[ch]
        arrived(relay[ch].at[0], "rs", ch * 3)
        p[1, row_b] = (p[1, row_b].astype(F32) + relay[ch][0].astype(F32)).astype(BF)
        send(p.at[1, row_b], recv_m[ch].at[row_b], sems("rs", ch * 3 + 2, ("r", ch)), dev_y[0])
        arrived(relay[ch].at[1], "rs", ch * 3 + 1)
        p[2, row_a] = (p[2, row_a].astype(F32) + relay[ch][1].astype(F32)).astype(BF)
        send(p.at[2, row_a], recv_p[ch].at[row_a], sems("rs", ch * 3 + 2, ("r", ch)), dev_y[1])

    def r2(ch):
        arrived(part[ch].at[0:2], "rs", ch * 3 + 2)
        col = pl.ds(STARTS[ch], WIDTHS[ch])
        eg_out[:, col] = eg_out[:, col] + (recv_m[ch][...].astype(F32) + recv_p[ch][...].astype(F32))

    def group_dev(n):
        i, j, k = GROUP[n]
        tx, tc, tz = up(xl, i, NXL), up(c, j, NCORE), up(z, k, NZ)
        return tx, tc, tz, {"xl": tx, "z": tz, "c": tc}

    def hr_send():
        hret[...] = acch[...].astype(BF).reshape(hret.shape)
        for n in range(1, len(GROUP)):
            tx, tc, tz, dev = group_dev(n)
            send(hret.at[tx, tc, tz], rbuf.at[slot], sems("hr", 0, "hr"), dev)
        pltpu.make_async_copy(hret.at[xl, c, z], rbuf.at[slot], r["hr"].at[0]).start()

    def table_flip():
        pick_t[...] = pick[...].reshape(N_SLOT * tok, pairs).T

    def hr_wait():
        arrived(rbuf, "hr", 0)
        scale = coef[...].reshape(N_SLOT * tok, 128)
        for n in range(hid // 256):
            halves = []
            for j in range(2):
                rows = rbuf[:, :, n * 256 + j * 128 : n * 256 + (j + 1) * 128]
                rows = rows.reshape(N_SLOT * tok, 128).astype(F32) * scale
                halves.append(rows.astype(BF))
            rows = jnp.concatenate(halves, axis=1)
            back = jnp.dot(pick_t[...], rows, preferred_element_type=F32)
            hg_out[:, n * 256 : (n + 1) * 256] = back.astype(BF)

    def d0a():
        d_local().start()
        f_local().start()
        lbuf[y, xh] = lsend[...]
        for i in range(1, NY):
            ty = up(y, i, NY)
            dev = {"y": ty}
            send(x_cols(ty, 1 - xh), xfwd.at[y], sems("dx", 1, "dx"), dev)
            send(lsend, lbuf.at[y, xh], sems("dl", 0, "dl"), dev)
            send(x_cols(ty, xh), xbuf.at[y, xh], sems("dx", 0, "dx"), dev)

    def d0b():
        arrived(xfwd, "dx", 1)
        arrived(lbuf.at[0:3, xh], "dl", 0)
        for s in range(2):
            send(xfwd.at[2 * s : 2 * s + 2], xrel.at[s], sems("xr", s, "dxf"), dev_x[s])
        send(lbuf.at[:, xh], lbuf.at[:, xh], sems("dl", 1, "dlf"), {"xh": 1 - xh})

    def d0c():
        for s in range(2):
            arrived(xrel.at[s], "xr", s)
            dst = xbuf.at[pl.ds(2 * s, 2), (xm, xp)[s] // NXL]
            send(xrel.at[s], dst, sems("dx", 0, "dxf"), dev_x[s])

    def d1():
        arrived(xbuf, "dx", 0)
        arrived(lbuf.at[:, xh], "dl", 1)
        n_tok = NY * NXH * tok

        def body(n, carry):
            col = pl.ds(pl.multiple_of(n * 128, 128), 128)
            xt = xbuf[:, :, :, col].reshape(n_tok, 128).T
            dpart[col, :] = jnp.dot(
                xt, lbuf[...].reshape(n_tok, lbuf.shape[-1]), preferred_element_type=F32
            )
            return carry

        lax.fori_loop(0, dcols // 128, body, 0)
        for n in range(N_SLOT):
            dsend[n] = dpart[n * drows : (n + 1) * drows].astype(BF)
        for n in range(1, len(GROUP)):
            tx, tc, tz, dev = group_dev(n)
            send(dsend.at[tz * 4 + tx * 2 + tc], drecv.at[slot], sems("ds", 0, "ds"), dev)
        pltpu.make_async_copy(dsend.at[slot], drecv.at[slot], r["ds"].at[0]).start()

    def d2():
        arrived(drecv, "ds", 0)
        mine = dpart[pl.ds(pl.multiple_of(slot * drows, 8), drows)]
        total = mine - drecv[slot].astype(F32)
        for n in range(len(GROUP)):
            total = total + drecv[n].astype(F32)
        dg_out[...] = total

    def sendwait():
        for ch in range(N_CHUNK):
            gone(gbuf[ch].at[0:3, c, z], ("a", ch))
            gone(gbuf[ch].at[0:3, c], ("b", ch))
            gone(gbuf[ch].at[:, c], ("d", ch))
            gone(part[ch], ("r", ch))
        gone(ht.at[0 : ht.shape[0] // 32 * 31], "h")
        gone(wbuf.at[0, pl.ds(0, (len(GROUP) - 1) * tok), pl.ds(0, hid)], "hr")
        gone(dsend.at[0 : N_SLOT - 1], "ds")
        gone(xbuf.at[0:3], "dx")
        gone(xbuf, "dxf")
        gone(lbuf.at[0:3, xh], "dl")
        gone(lbuf.at[:, xh], "dlf")

    greet()
    saved_copy().start()
    own_copy(0).start()
    own_copy(1).start()
    own_copy(2).start()
    own_copy(3).start()
    own_copy(4).start()
    w_copy(0).start()
    w_copy(1).start()
    prep()
    own_wait()
    bar()
    h_send(16, 24, 0)
    s0(1)
    h_send(16, 24, 2)
    h_send(24, 31, 0)
    s0(0)
    h_send(8, 16, 1)
    table_flip()
    h_send(16, 24, 1)
    h_send(0, 8, 0)
    d0a()
    h_send(8, 16, 0)
    s2(0)
    s0(2)
    h_send(0, 8, 1)
    s1(1)
    h_send(24, 31, 1)
    s3(0)
    h_build(0)
    s2(1)
    h_send(0, 8, 2)
    h_build(1)
    h_send(8, 16, 2)
    s1(2)
    s4(0)
    s5(0)
    m0(0)
    r0a(0)
    h_send(24, 31, 2)
    m0(1)
    s3(1)
    s0(3)
    s2(2)
    mm2(0)
    s0(4)
    r0b(0)
    s4(1)
    h_build(2)
    r1(0)
    s5(1)
    mm1(1)
    s1(3)
    r0a(1)
    s3(2)
    s1(4)
    s2(3)
    r0b(1)
    mm2(1)
    s4(2)
    r1(1)
    m0(2)
    r2(0)
    s2(4)
    s5(2)
    mm1(2)
    s3(3)
    r0a(2)
    r0b(2)
    mm2(2)
    s4(3)
    s3(4)
    d0b()
    s5(3)
    mm1(3)
    s4(4)
    d0c()
    mm2(3)
    r0b(3)
    s5(4)
    mm2(4)
    hr_send()
    r2(1)
    mm1(4)
    r0a(3)
    r1(2)
    r0b(4)
    d1()
    r2(2)
    r0a(4)
    r1(3)
    r1(4)
    r2(3)
    d2()
    hr_wait()
    r2(4)
    sendwait()


def exchange(ids, home, live, gates, lat, g, sv, w, xin):
    tok, d = g.shape
    pairs, hid = sv.shape
    kvr = lat.shape[1]
    frows = hid // 8
    drows = d // 128
    dma = pltpu.SemaphoreType.DMA
    v = pltpu.VMEM
    smem, vmem, hbm = (
        pl.BlockSpec(memory_space=m) for m in (pltpu.SMEM, pltpu.VMEM, pl.ANY)
    )
    ins = {
        "ids": vmem, "home": smem, "live": smem, "gates": vmem, "lat": vmem,
        "g": hbm, "sv": hbm, "w": hbm, "x": hbm,
    }
    outs = ("hg_out", "eg_out", "dg_out")
    scratch = {
        "hs": v((NXH, N_SLOT, tok, hid // NXH), BF),
        "hbuf": v((NX, NCORE, NZ, tok, hid // NXH), BF),
        "ht": v((hid // NXH, len(PLANE) * tok), BF),
        "wbuf": v((2, hid, max(WIDTHS)), BF),
        "acch": v((len(GROUP) * tok, hid), F32),
        "hret": v((NXL, NCORE, NZ, tok, hid), BF),
        "rbuf": v((N_SLOT, tok, hid), BF),
        "saved": v((pairs, hid), BF),
        "pick": v((N_SLOT, tok, pairs), BF),
        "pick_t": v((pairs, N_SLOT * tok), BF),
        "coef": v((N_SLOT, tok, 128), F32),
        "flip": v((2, 128, 128), F32),
        "xbuf": v((NY, NXH, tok, d // 8), BF),
        "xfwd": v((NY, tok, d // 8), BF),
        "xrel": v((2, NY // 2, tok, d // 8), BF),
        "lsend": v((tok, kvr), BF),
        "lbuf": v((NY, NXH, tok, kvr), BF),
        "dpart": v((d // 8, kvr), F32),
        "dsend": v((N_SLOT, drows, kvr), BF),
        "drecv": v((N_SLOT, drows, kvr), BF),
    }
    for i, width in enumerate(WIDTHS):
        scratch["gbuf" + str(i)] = v((NX, NCORE, NZ, tok, width), BF)
        scratch["part" + str(i)] = v((NY - 1, frows, width), BF)
        scratch["relay" + str(i)] = v((2, frows // 2, width), BF)
        scratch["recv_p" + str(i)] = v((frows, width), BF)
        scratch["recv_m" + str(i)] = v((frows, width), BF)
    counts = {
        "a1": N_CHUNK * 4, "a2": N_CHUNK, "b1": N_CHUNK * 4, "b2": N_CHUNK, "dd": N_CHUNK,
        "h": len(PARTS), "rs": N_CHUNK * 3, "hr": 1, "dx": 2, "xr": 2, "dl": 2, "ds": 1,
        "loc": 2, "w_sem": 2, "out": N_CHUNK * 4 + 7,
    }
    for name, count in counts.items():
        scratch[name] = dma((count,))
    names = tuple(ins) + outs + tuple(scratch)

    def body(*refs):
        kernel(names, *refs)

    return pl.pallas_call(
        body,
        out_shape=(
            v((pairs, hid), BF),
            v((frows, d), F32),
            v((drows, kvr), F32),
        ),
        in_specs=list(ins.values()),
        out_specs=(vmem, vmem, vmem),
        scratch_shapes=list(scratch.values()),
        compiler_params=pltpu.CompilerParams(
            collective_id=0, has_side_effects=True, vmem_limit_bytes=56 * 1024 * 1024
        ),
        name="exchange",
    )(ids, home, live, gates, lat, g, sv, w, xin)


def leave(hg, eg, dg):
    pieces = 4
    step = eg.shape[0] // pieces

    def body(hg_in, eg_in, dg_in, hg_out, eg_out, dg_out, sem):
        copies = [
            pltpu.make_async_copy(
                eg_in.at[pl.ds(i * step, step)], eg_out.at[pl.ds(i * step, step)], sem.at[i]
            )
            for i in range(pieces)
        ]
        copies.append(pltpu.make_async_copy(hg_in, hg_out, sem.at[pieces]))
        copies.append(pltpu.make_async_copy(dg_in, dg_out, sem.at[pieces + 1]))
        for copy in copies:
            copy.start()
        for copy in copies:
            copy.wait()

    return pl.pallas_call(
        body,
        out_shape=tuple(jax.ShapeDtypeStruct(a.shape, a.dtype) for a in (hg, eg, dg)),
        in_specs=[pl.BlockSpec(memory_space=pltpu.VMEM)] * 3,
        out_specs=(pl.BlockSpec(memory_space=pl.ANY),) * 3,
        scratch_shapes=[pltpu.SemaphoreType.DMA((pieces + 2,))],
        compiler_params=pltpu.CompilerParams(vmem_limit_bytes=1024 * 1024),
        name="leave",
    )(hg, eg, dg)


def on_device(
    expert_ids,
    expert_home,
    live_tokens,
    gate_weights,
    output_grad,
    saved_hidden,
    down_weight,
    dense_input,
    latent_grad,
):
    tok, topk = expert_ids.shape
    hid = saved_hidden.shape[2]
    hg, eg, dg = exchange(
        expert_ids.T,
        expert_home,
        live_tokens,
        gate_weights.T,
        latent_grad,
        output_grad,
        saved_hidden.reshape(tok * topk, hid),
        down_weight[0],
        dense_input,
    )
    hg, eg, dg = leave(hg, eg, dg)
    return hg.reshape(tok, topk, hid), eg[None], dg


def solution(mesh):
    torus = Mesh(mesh.devices.reshape(4, 2, 4, 2, 2), ALL)
    in_specs = (
        P(ALL, None),
        P(),
        P(ALL),
        P(ALL, None),
        P(ALL, None),
        P(ALL, None, None),
        P(EXPERT, None, None),
        P(ALL, None),
        P(ALL, None),
    )
    out_specs = (P(ALL, None, None), P(EXPERT, DP, None), P(ALL, None))
    return jax.shard_map(
        on_device, mesh=torus, in_specs=in_specs, out_specs=out_specs, check_vma=False
    )
```

```python
import jax
import jax.numpy as jnp
from jax import lax
from jax.experimental import pallas as pl
from jax.experimental.pallas import tpu as pltpu
from jax.sharding import Mesh
from jax.sharding import PartitionSpec as P

DP = ("y", "xh")
EXPERT = ("z", "xl", "c")
ALL = ("y", "xh", "z", "xl", "c")
MESH = pl.DeviceIdType.MESH
NY, NX, NZ, NCORE, NXH, NXL = 4, 4, 4, 2, 2, 2
N_SLOT = 16
BF = jnp.bfloat16
F32 = jnp.float32
WIDTHS = (1024, 1536, 2048, 1536, 1024)
N_CHUNK = len(WIDTHS)
STARTS = tuple(sum(WIDTHS[:i]) for i in range(N_CHUNK))
PLANE = [(i, j, k) for i in range(NX) for j in range(NCORE) for k in range(NZ)]
GROUP = [(i, j, k) for i in range(NXL) for j in range(NCORE) for k in range(NZ)]
ORDER = (2, 1, 3, 0)
PARTS = ((0, 1), (1, 3), (3, 4))


def up(v, k, n):
    return lax.rem(v + k, n)


def kernel(names, *all_refs):
    r = dict(zip(names, all_refs))
    ids, home, live, gates, lat = (r[k] for k in ("ids", "home", "live", "gates", "lat"))
    g_hbm, sv_hbm, w_hbm, x_hbm = (r[k] for k in ("g", "sv", "w", "x"))
    hg_out, eg_out, dg_out = r["hg_out"], r["eg_out"], r["dg_out"]
    gbuf, part, relay, recv_p, recv_m = (
        [r[k + str(i)] for i in range(N_CHUNK)] for k in ("gbuf", "part", "relay", "recv_p", "recv_m")
    )
    hs, hbuf, ht, wbuf, acch, hret, rbuf = (
        r[k] for k in ("hs", "hbuf", "ht", "wbuf", "acch", "hret", "rbuf")
    )
    saved, pick, pick_t, coef, flip = (r[k] for k in ("saved", "pick", "pick_t", "coef", "flip"))
    xbuf, xfwd, xrel, lsend, lbuf, dpart, dsend, drecv = (
        r[k] for k in ("xbuf", "xfwd", "xrel", "lsend", "lbuf", "dpart", "dsend", "drecv")
    )

    y = lax.axis_index("y")
    xh = lax.axis_index("xh")
    z = lax.axis_index("z")
    xl = lax.axis_index("xl")
    c = lax.axis_index("c")
    x = xh * NXL + xl
    slot = z * 4 + xl * 2 + c
    tok = g_hbm.shape[0]
    half_tok = tok // 2
    topk = ids.shape[0]
    pairs = tok * topk
    frows = ht.shape[0] // NY
    hrow = frows // 2
    hid = w_hbm.shape[0]
    dcols = xbuf.shape[-1]
    drows = drecv.shape[1]
    rows_of = (pl.ds(0, half_tok), pl.ds(half_tok, half_tok))

    def at_x(v):
        return {"xh": v // NXL, "xl": lax.rem(v, NXL)}

    xp, xm, x2 = up(x, 1, NX), up(x, NX - 1, NX), up(x, 2, NX)
    zp, zm, z2 = up(z, 1, NZ), up(z, NZ - 1, NZ), up(z, 2, NZ)
    yp, ym = up(y, 1, NY), up(y, NY - 1, NY)
    dev_x = (at_x(xp), at_x(xm), at_x(x2))
    dev_z = ({"z": zp}, {"z": zm}, {"z": z2})
    dev_y = ({"y": yp}, {"y": ym})
    sibling = {"c": 1 - c}
    classes = {}

    def sems(name, at, out):
        return r["out"].at[classes.setdefault(out, len(classes))], r[name].at[at]

    def remote(src, dst, pair, dev):
        return pltpu.make_async_remote_copy(
            src_ref=src,
            dst_ref=dst,
            send_sem=pair[0],
            recv_sem=pair[1],
            device_id=dev,
            device_id_type=MESH,
        )

    def send(src, dst, pair, dev):
        remote(src, dst, pair, dev).start()

    def arrived(ref, name, at):
        sem = r[name].at[at]
        remote(ref, ref, (sem, sem), sibling).wait_recv()

    def gone(ref, out):
        sem = r["out"].at[classes[out]]
        remote(ref, ref, (sem, sem), sibling).wait_send()

    def plane_dev(n):
        i, j, k = PLANE[n]
        tx, tc, tz = up(x, i, NX), up(c, j, NCORE), up(z, k, NZ)
        return tx, tc, tz, {"xh": tx // NXL, "xl": lax.rem(tx, NXL), "z": tz, "c": tc}

    barrier = pltpu.get_barrier_semaphore()

    def greet():
        for n in range(1, len(PLANE)):
            pl.semaphore_signal(barrier, inc=1, device_id=plane_dev(n)[3], device_id_type=MESH)
        for i in range(1, NY):
            pl.semaphore_signal(barrier, inc=1, device_id={"y": up(y, i, NY)}, device_id_type=MESH)

    def bar():
        pl.semaphore_wait(barrier, len(PLANE) - 1 + NY - 1)

    def own_copy(ch):
        return pltpu.make_async_copy(
            g_hbm.at[:, pl.ds(STARTS[ch], WIDTHS[ch])], gbuf[ch].at[x, c, z], r["loc"].at[0]
        )

    def saved_copy():
        return pltpu.make_async_copy(sv_hbm, saved, r["loc"].at[1])

    def h_local(which):
        lo, hi = PARTS[which]
        col = pl.ds(lo * frows, (hi - lo) * frows)
        return pltpu.make_async_copy(
            hs.at[xh, slot, :, col], hbuf.at[x, c, z, :, col], r["h"].at[which]
        )

    def x_cols(ty, th):
        return x_hbm.at[:, pl.ds(pl.multiple_of((ty * 2 + th) * dcols, 128), dcols)]

    def d_local():
        return pltpu.make_async_copy(x_cols(y, xh), xbuf.at[y, xh], r["dx"].at[0])

    def f_local():
        return pltpu.make_async_copy(x_cols(y, 1 - xh), xfwd.at[y], r["dx"].at[1])

    def w_copy(ch):
        return pltpu.make_async_copy(
            w_hbm.at[:, pl.ds(STARTS[ch], WIDTHS[ch])],
            wbuf.at[ch % 2, :, pl.ds(0, WIDTHS[ch])],
            r["w_sem"].at[ch % 2],
        )

    def prep():
        homes = jnp.zeros(ids.shape, F32)
        for e in range(N_SLOT):
            homes = jnp.where(ids[...] == e, home[e].astype(F32), homes)
        is_live = lax.broadcasted_iota(jnp.int32, ids.shape, 1) < live[0]
        flip[...] = jnp.zeros_like(flip)
        flip[0, 0:topk, 0:tok] = homes
        flip[1, 0:topk, 0:tok] = jnp.where(is_live, gates[...], jnp.zeros_like(gates))
        home_t = flip[0].T[0:tok]
        scale_t = flip[1].T[0:tok]
        lane = lax.broadcasted_iota(jnp.int32, (128, pairs), 1)
        row = lax.broadcasted_iota(jnp.int32, (128, pairs), 0)
        spread = jnp.where(lax.rem(lane, topk) == row, 1.0, 0.0).astype(BF)
        wide = jnp.dot(home_t.astype(BF), spread, preferred_element_type=F32)
        lane = lax.broadcasted_iota(jnp.int32, (tok, pairs), 1)
        row = lax.broadcasted_iota(jnp.int32, (tok, pairs), 0)
        wide = jnp.where(lane // topk == row, wide, -1.0)
        column = lax.broadcasted_iota(jnp.int32, (tok, 128), 1)
        for s in range(N_SLOT):
            pick[s] = jnp.where(wide == float(s), 1.0, 0.0).astype(BF)
            mine = jnp.where((home_t == float(s)) & (column < topk), scale_t, 0.0)
            coef[s] = jnp.broadcast_to(jnp.sum(mine, axis=1, keepdims=True), (tok, 128))
        token = lax.broadcasted_iota(jnp.int32, lat.shape, 0)
        lsend[...] = jnp.where(token < live[0], lat[...], jnp.zeros_like(lat))
        saved_copy().wait()
        table = pick[...].reshape(N_SLOT * tok, pairs)
        scale = coef[...].reshape(N_SLOT * tok, 128)
        for n, k in enumerate(ORDER):
            col = pl.ds(pl.multiple_of(up(y, k, NY) * NXH * frows, NXH * frows), NXH * frows)
            rows = jnp.dot(table, saved[:, col], preferred_element_type=F32)
            for j in range(NXH):
                scaled = (rows[:, j * frows : (j + 1) * frows] * scale).astype(BF)
                hs[j, :, :, n * frows : (n + 1) * frows] = scaled.reshape(N_SLOT, tok, frows)

    def lanes(ch, h):
        return pl.ds(h * (WIDTHS[ch] // 2), WIDTHS[ch] // 2)

    def direct(ch):
        return ch == 0

    def own_wait():
        pltpu.make_async_copy(g_hbm, g_hbm, r["loc"].at[0]).wait()

    def s0(ch):
        for h in range(2):
            ref = gbuf[ch].at[x, c, z, :, lanes(ch, h)]
            for s in range(3 if direct(ch) else 2):
                at = 0 if direct(ch) else ch * 4 + h * 2 + s
                send(ref, ref, sems("a1", at, ("a", ch)), (dev_x, dev_z)[h][s])

    def s1(ch):
        for h in range(2):
            for s in range(2):
                if h == 0:
                    blk = gbuf[ch].at[(xm, xp)[s], c, z]
                else:
                    blk = gbuf[ch].at[x, c, (zm, zp)[s]]
                dev = (dev_x, dev_z)[h][s]
                arrived(blk.at[:, lanes(ch, h)], "a1", ch * 4 + h * 2 + s)
                ref = blk.at[rows_of[s], lanes(ch, h)]
                send(ref, ref, sems("a2", ch, ("a", ch)), dev)

    def line(ch, h, other):
        if h == 0:
            return gbuf[ch].at[:, c, other, :, lanes(ch, 0)]
        return gbuf[ch].at[other, c, :, :, lanes(ch, 1)]

    def line_half(ch, h, other, s):
        if h == 0:
            return gbuf[ch].at[:, c, other, rows_of[s], lanes(ch, 0)]
        return gbuf[ch].at[other, c, :, rows_of[s], lanes(ch, 1)]

    def s2(ch):
        if direct(ch):
            arrived(gbuf[ch].at[0:3, c, z], "a1", 0)
        else:
            arrived(gbuf[ch].at[0, c, z], "a2", ch)
        for h in range(2):
            ref = line(ch, h, (z, x)[h])
            for s in range(2):
                send(ref, ref, sems("b1", ch * 4 + h * 2 + s, ("b", ch)), (dev_z, dev_x)[h][s])
            send(ref, ref, sems("dd", ch, ("d", ch)), sibling)

    def s3(ch):
        for h in range(2):
            for s in range(2):
                other = ((zm, zp), (xm, xp))[h][s]
                dev = (dev_z, dev_x)[h][s]
                ref = line(ch, h, other)
                arrived(ref, "b1", ch * 4 + h * 2 + s)
                fwd = line_half(ch, h, other, s)
                send(fwd, fwd, sems("b2", ch, ("b", ch)), dev)
                send(ref, ref, sems("dd", ch, ("d", ch)), sibling)

    def s4(ch):
        arrived(gbuf[ch].at[:, c, z], "b2", ch)
        for h in range(2):
            ref = line(ch, h, (z2, x2)[h])
            send(ref, ref, sems("dd", ch, ("d", ch)), sibling)

    def s5(ch):
        arrived(gbuf[ch].at[:, 1 - c], "dd", ch)

    def h_send(first, last, which):
        if first == 0:
            h_local(which).start()
        lo, hi = PARTS[which]
        col = pl.ds(lo * frows, (hi - lo) * frows)
        for m in range(first, last):
            n = ((m + 1) * 11) % len(PLANE)
            tx, tc, tz, dev = plane_dev(n)
            t_slot = tz * 4 + lax.rem(tx, NXL) * 2 + tc
            src = hs.at[tx // NXL, t_slot, :, col]
            send(src, hbuf.at[x, c, z, :, col], sems("h", which, "h"), dev)

    def h_build(which):
        lo, hi = PARTS[which]
        col = pl.ds(lo * frows, (hi - lo) * frows)
        arrived(hbuf.at[:, :, :, :, col], "h", which)
        n_tok = NCORE * NZ * tok
        for k in range(lo, hi):
            for i in range(NX):
                blk = hbuf[i, :, :, :, k * frows : (k + 1) * frows].reshape(n_tok, frows)
                ht[pl.ds(k * frows, frows), pl.ds(i * n_tok, n_tok)] = blk.T

    def mm1(ch, lo=0, hi=NY):
        def body(n, carry):
            col = pl.ds(pl.multiple_of(n * 256, 256), 256)
            g = gbuf[ch][:, :, :, :, col].reshape(len(PLANE) * tok, 256)
            p = jnp.dot(ht[lo * frows : hi * frows], g, preferred_element_type=F32)
            for k in range(lo, hi):
                rows = p[(k - lo) * frows : (k - lo + 1) * frows]
                if k == NY - 1:
                    eg_out[:, pl.ds(pl.multiple_of(STARTS[ch] + n * 256, 256), 256)] = rows
                else:
                    part[ch][k, :, col] = rows.astype(BF)
            return carry

        lax.fori_loop(0, WIDTHS[ch] // 256, body, 0)

    def m0(which):
        mm1(0, *PARTS[which])

    def mm2(ch):
        w_copy(ch).wait()

        def body(n, carry):
            row = pl.ds(pl.multiple_of(n * 256, 256), 256)
            g = gbuf[ch][pl.ds(xh * NXL, NXL)].reshape(len(GROUP) * tok, WIDTHS[ch])
            w = wbuf[ch % 2, row, pl.ds(0, WIDTHS[ch])]
            p = lax.dot_general(g, w, (((1,), (1,)), ((), ())), preferred_element_type=F32)
            if ch == 0:
                acch[:, row] = p
            else:
                acch[:, row] = acch[:, row] + p
            return carry

        lax.fori_loop(0, hid // 256, body, 0)
        if ch + 2 < N_CHUNK:
            w_copy(ch + 2).start()

    row_a, row_b = pl.ds(0, hrow), pl.ds(hrow, hrow)

    def r0a(ch):
        p = part[ch]
        send(p.at[0, row_b], relay[ch].at[0], sems("rs", ch * 3 + 0, ("r", ch)), dev_y[0])
        send(p.at[0, row_a], relay[ch].at[1], sems("rs", ch * 3 + 1, ("r", ch)), dev_y[1])

    def r0b(ch):
        p = part[ch]
        send(p.at[1, row_a], recv_m[ch].at[row_a], sems("rs", ch * 3 + 2, ("r", ch)), dev_y[0])
        send(p.at[2, row_b], recv_p[ch].at[row_b], sems("rs", ch * 3 + 2, ("r", ch)), dev_y[1])

    def r1(ch):
        p = part[ch]
        arrived(relay[ch].at[0], "rs", ch * 3)
        p[1, row_b] = (p[1, row_b].astype(F32) + relay[ch][0].astype(F32)).astype(BF)
        send(p.at[1, row_b], recv_m[ch].at[row_b], sems("rs", ch * 3 + 2, ("r", ch)), dev_y[0])
        arrived(relay[ch].at[1], "rs", ch * 3 + 1)
        p[2, row_a] = (p[2, row_a].astype(F32) + relay[ch][1].astype(F32)).astype(BF)
        send(p.at[2, row_a], recv_p[ch].at[row_a], sems("rs", ch * 3 + 2, ("r", ch)), dev_y[1])

    def r2(ch):
        arrived(part[ch].at[0:2], "rs", ch * 3 + 2)
        col = pl.ds(STARTS[ch], WIDTHS[ch])
        eg_out[:, col] = eg_out[:, col] + (recv_m[ch][...].astype(F32) + recv_p[ch][...].astype(F32))

    def group_dev(n):
        i, j, k = GROUP[n]
        tx, tc, tz = up(xl, i, NXL), up(c, j, NCORE), up(z, k, NZ)
        return tx, tc, tz, {"xl": tx, "z": tz, "c": tc}

    def hr_send():
        hret[...] = acch[...].astype(BF).reshape(hret.shape)
        for n in range(1, len(GROUP)):
            tx, tc, tz, dev = group_dev(n)
            send(hret.at[tx, tc, tz], rbuf.at[slot], sems("hr", 0, "hr"), dev)
        pltpu.make_async_copy(hret.at[xl, c, z], rbuf.at[slot], r["hr"].at[0]).start()

    def table_flip():
        pick_t[...] = pick[...].reshape(N_SLOT * tok, pairs).T

    def hr_wait():
        arrived(rbuf, "hr", 0)
        scale = coef[...].reshape(N_SLOT * tok, 128)
        for n in range(hid // 256):
            halves = []
            for j in range(2):
                rows = rbuf[:, :, n * 256 + j * 128 : n * 256 + (j + 1) * 128]
                rows = rows.reshape(N_SLOT * tok, 128).astype(F32) * scale
                halves.append(rows.astype(BF))
            rows = jnp.concatenate(halves, axis=1)
            back = jnp.dot(pick_t[...], rows, preferred_element_type=F32)
            hg_out[:, n * 256 : (n + 1) * 256] = back.astype(BF)

    def d0a():
        d_local().start()
        f_local().start()
        lbuf[y, xh] = lsend[...]
        for i in range(1, NY):
            ty = up(y, i, NY)
            dev = {"y": ty}
            send(x_cols(ty, 1 - xh), xfwd.at[y], sems("dx", 1, "dx"), dev)
            send(lsend, lbuf.at[y, xh], sems("dl", 0, "dl"), dev)
            send(x_cols(ty, xh), xbuf.at[y, xh], sems("dx", 0, "dx"), dev)

    def d0b():
        arrived(xfwd, "dx", 1)
        arrived(lbuf.at[0:3, xh], "dl", 0)
        for s in range(2):
            send(xfwd.at[2 * s : 2 * s + 2], xrel.at[s], sems("xr", s, "dxf"), dev_x[s])
        send(lbuf.at[:, xh], lbuf.at[:, xh], sems("dl", 1, "dlf"), {"xh": 1 - xh})

    def d0c():
        for s in range(2):
            arrived(xrel.at[s], "xr", s)
            dst = xbuf.at[pl.ds(2 * s, 2), (xm, xp)[s] // NXL]
            send(xrel.at[s], dst, sems("dx", 0, "dxf"), dev_x[s])

    def d1():
        arrived(xbuf, "dx", 0)
        arrived(lbuf.at[:, xh], "dl", 1)
        n_tok = NY * NXH * tok

        def body(n, carry):
            col = pl.ds(pl.multiple_of(n * 128, 128), 128)
            xt = xbuf[:, :, :, col].reshape(n_tok, 128).T
            dpart[col, :] = jnp.dot(
                xt, lbuf[...].reshape(n_tok, lbuf.shape[-1]), preferred_element_type=F32
            )
            return carry

        lax.fori_loop(0, dcols // 128, body, 0)
        for n in range(N_SLOT):
            dsend[n] = dpart[n * drows : (n + 1) * drows].astype(BF)
        for n in range(1, len(GROUP)):
            tx, tc, tz, dev = group_dev(n)
            send(dsend.at[tz * 4 + tx * 2 + tc], drecv.at[slot], sems("ds", 0, "ds"), dev)
        pltpu.make_async_copy(dsend.at[slot], drecv.at[slot], r["ds"].at[0]).start()

    def d2():
        arrived(drecv, "ds", 0)
        mine = dpart[pl.ds(pl.multiple_of(slot * drows, 8), drows)]
        total = mine - drecv[slot].astype(F32)
        for n in range(len(GROUP)):
            total = total + drecv[n].astype(F32)
        dg_out[...] = total

    def sendwait():
        for ch in range(N_CHUNK):
            gone(gbuf[ch].at[0:3, c, z], ("a", ch))
            gone(gbuf[ch].at[0:3, c], ("b", ch))
            gone(gbuf[ch].at[:, c], ("d", ch))
            gone(part[ch], ("r", ch))
        gone(ht.at[0 : ht.shape[0] // 32 * 31], "h")
        gone(wbuf.at[0, pl.ds(0, (len(GROUP) - 1) * tok), pl.ds(0, hid)], "hr")
        gone(dsend.at[0 : N_SLOT - 1], "ds")
        gone(xbuf.at[0:3], "dx")
        gone(xbuf, "dxf")
        gone(lbuf.at[0:3, xh], "dl")
        gone(lbuf.at[:, xh], "dlf")

    greet()
    saved_copy().start()
    own_copy(0).start()
    own_copy(1).start()
    own_copy(2).start()
    own_copy(3).start()
    own_copy(4).start()
    w_copy(0).start()
    w_copy(1).start()
    prep()
    own_wait()
    bar()
    h_send(16, 24, 0)
    s0(1)
    h_send(16, 24, 2)
    h_send(24, 31, 0)
    s0(0)
    h_send(8, 16, 1)
    table_flip()
    h_send(16, 24, 1)
    h_send(0, 8, 0)
    d0a()
    h_send(8, 16, 0)
    s2(0)
    s0(2)
    h_send(0, 8, 1)
    s1(1)
    h_send(24, 31, 1)
    s3(0)
    h_build(0)
    s2(1)
    h_send(0, 8, 2)
    h_build(1)
    h_send(8, 16, 2)
    s1(2)
    s4(0)
    s5(0)
    m0(0)
    r0a(0)
    h_send(24, 31, 2)
    m0(1)
    s3(1)
    s0(3)
    s2(2)
    mm2(0)
    s0(4)
    r0b(0)
    s4(1)
    h_build(2)
    r1(0)
    s5(1)
    mm1(1)
    s1(3)
    r0a(1)
    s3(2)
    s1(4)
    s2(3)
    r0b(1)
    mm2(1)
    s4(2)
    r1(1)
    m0(2)
    r2(0)
    s2(4)
    s5(2)
    mm1(2)
    s3(3)
    r0a(2)
    r0b(2)
    mm2(2)
    s4(3)
    s3(4)
    d0b()
    s5(3)
    mm1(3)
    r0a(3)
    r0b(3)
    s4(4)
    d0c()
    mm2(3)
    s5(4)
    mm1(4)
    r0a(4)
    r0b(4)
    mm2(4)
    hr_send()
    r1(2)
    d1()
    r1(3)
    r2(1)
    r2(2)
    r1(4)
    r2(3)
    d2()
    hr_wait()
    r2(4)
    sendwait()


def exchange(ids, home, live, gates, lat, g, sv, w, xin):
    tok, d = g.shape
    pairs, hid = sv.shape
    kvr = lat.shape[1]
    frows = hid // 8
    drows = d // 128
    dma = pltpu.SemaphoreType.DMA
    v = pltpu.VMEM
    smem, vmem, hbm = (
        pl.BlockSpec(memory_space=m) for m in (pltpu.SMEM, pltpu.VMEM, pl.ANY)
    )
    ins = {
        "ids": vmem, "home": smem, "live": smem, "gates": vmem, "lat": vmem,
        "g": hbm, "sv": hbm, "w": hbm, "x": hbm,
    }
    outs = ("hg_out", "eg_out", "dg_out")
    scratch = {
        "hs": v((NXH, N_SLOT, tok, hid // NXH), BF),
        "hbuf": v((NX, NCORE, NZ, tok, hid // NXH), BF),
        "ht": v((hid // NXH, len(PLANE) * tok), BF),
        "wbuf": v((2, hid, max(WIDTHS)), BF),
        "acch": v((len(GROUP) * tok, hid), F32),
        "hret": v((NXL, NCORE, NZ, tok, hid), BF),
        "rbuf": v((N_SLOT, tok, hid), BF),
        "saved": v((pairs, hid), BF),
        "pick": v((N_SLOT, tok, pairs), BF),
        "pick_t": v((pairs, N_SLOT * tok), BF),
        "coef": v((N_SLOT, tok, 128), F32),
        "flip": v((2, 128, 128), F32),
        "xbuf": v((NY, NXH, tok, d // 8), BF),
        "xfwd": v((NY, tok, d // 8), BF),
        "xrel": v((2, NY // 2, tok, d // 8), BF),
        "lsend": v((tok, kvr), BF),
        "lbuf": v((NY, NXH, tok, kvr), BF),
        "dpart": v((d // 8, kvr), F32),
        "dsend": v((N_SLOT, drows, kvr), BF),
        "drecv": v((N_SLOT, drows, kvr), BF),
    }
    for i, width in enumerate(WIDTHS):
        scratch["gbuf" + str(i)] = v((NX, NCORE, NZ, tok, width), BF)
        scratch["part" + str(i)] = v((NY - 1, frows, width), BF)
        scratch["relay" + str(i)] = v((2, frows // 2, width), BF)
        scratch["recv_p" + str(i)] = v((frows, width), BF)
        scratch["recv_m" + str(i)] = v((frows, width), BF)
    counts = {
        "a1": N_CHUNK * 4, "a2": N_CHUNK, "b1": N_CHUNK * 4, "b2": N_CHUNK, "dd": N_CHUNK,
        "h": len(PARTS), "rs": N_CHUNK * 3, "hr": 1, "dx": 2, "xr": 2, "dl": 2, "ds": 1,
        "loc": 2, "w_sem": 2, "out": N_CHUNK * 4 + 7,
    }
    for name, count in counts.items():
        scratch[name] = dma((count,))
    names = tuple(ins) + outs + tuple(scratch)

    def body(*refs):
        kernel(names, *refs)

    return pl.pallas_call(
        body,
        out_shape=(
            v((pairs, hid), BF),
            v((frows, d), F32),
            v((drows, kvr), F32),
        ),
        in_specs=list(ins.values()),
        out_specs=(vmem, vmem, vmem),
        scratch_shapes=list(scratch.values()),
        compiler_params=pltpu.CompilerParams(
            collective_id=0, has_side_effects=True, vmem_limit_bytes=56 * 1024 * 1024
        ),
        name="exchange",
    )(ids, home, live, gates, lat, g, sv, w, xin)


def leave(hg, eg, dg):
    pieces = 4
    step = eg.shape[0] // pieces

    def body(hg_in, eg_in, dg_in, hg_out, eg_out, dg_out, sem):
        copies = [
            pltpu.make_async_copy(
                eg_in.at[pl.ds(i * step, step)], eg_out.at[pl.ds(i * step, step)], sem.at[i]
            )
            for i in range(pieces)
        ]
        copies.append(pltpu.make_async_copy(hg_in, hg_out, sem.at[pieces]))
        copies.append(pltpu.make_async_copy(dg_in, dg_out, sem.at[pieces + 1]))
        for copy in copies:
            copy.start()
        for copy in copies:
            copy.wait()

    return pl.pallas_call(
        body,
        out_shape=tuple(jax.ShapeDtypeStruct(a.shape, a.dtype) for a in (hg, eg, dg)),
        in_specs=[pl.BlockSpec(memory_space=pltpu.VMEM)] * 3,
        out_specs=(pl.BlockSpec(memory_space=pl.ANY),) * 3,
        scratch_shapes=[pltpu.SemaphoreType.DMA((pieces + 2,))],
        compiler_params=pltpu.CompilerParams(vmem_limit_bytes=1024 * 1024),
        name="leave",
    )(hg, eg, dg)


def on_device(
    expert_ids,
    expert_home,
    live_tokens,
    gate_weights,
    output_grad,
    saved_hidden,
    down_weight,
    dense_input,
    latent_grad,
):
    tok, topk = expert_ids.shape
    hid = saved_hidden.shape[2]
    hg, eg, dg = exchange(
        expert_ids.T,
        expert_home,
        live_tokens,
        gate_weights.T,
        latent_grad,
        output_grad,
        saved_hidden.reshape(tok * topk, hid),
        down_weight[0],
        dense_input,
    )
    hg, eg, dg = leave(hg, eg, dg)
    return hg.reshape(tok, topk, hid), eg[None], dg


def solution(mesh):
    torus = Mesh(mesh.devices.reshape(4, 2, 4, 2, 2), ALL)
    in_specs = (
        P(ALL, None),
        P(),
        P(ALL),
        P(ALL, None),
        P(ALL, None),
        P(ALL, None, None),
        P(EXPERT, None, None),
        P(ALL, None),
        P(ALL, None),
    )
    out_specs = (P(ALL, None, None), P(EXPERT, DP, None), P(ALL, None))
    return jax.shard_map(
        on_device, mesh=torus, in_specs=in_specs, out_specs=out_specs, check_vma=False
    )
```

```python
import jax
import jax.numpy as jnp
from jax import lax
from jax.experimental import pallas as pl
from jax.experimental.pallas import tpu as pltpu
from jax.sharding import Mesh
from jax.sharding import PartitionSpec as P

DP = ("y", "xh")
EXPERT = ("z", "xl", "c")
ALL = ("y", "xh", "z", "xl", "c")
MESH = pl.DeviceIdType.MESH
NY, NX, NZ, NCORE, NXH, NXL = 4, 4, 4, 2, 2, 2
N_SLOT = 16
BF = jnp.bfloat16
F32 = jnp.float32
WIDTHS = (1536, 1536, 1792, 1280, 1024)
N_CHUNK = len(WIDTHS)
STARTS = tuple(sum(WIDTHS[:i]) for i in range(N_CHUNK))
PLANE = [(i, j, k) for i in range(NX) for j in range(NCORE) for k in range(NZ)]
GROUP = [(i, j, k) for i in range(NXL) for j in range(NCORE) for k in range(NZ)]
ORDER = (2, 1, 3, 0)
PARTS = ((0, 1), (1, 3), (3, 4))


def up(v, k, n):
    return lax.rem(v + k, n)


def kernel(names, *all_refs):
    r = dict(zip(names, all_refs))
    ids, home, live, gates, lat = (r[k] for k in ("ids", "home", "live", "gates", "lat"))
    g_hbm, sv_hbm, w_hbm, x_hbm = (r[k] for k in ("g", "sv", "w", "x"))
    hg_out, eg_out, dg_out = r["hg_out"], r["eg_out"], r["dg_out"]
    gbuf, part, relay, recv_p, recv_m = (
        [r[k + str(i)] for i in range(N_CHUNK)] for k in ("gbuf", "part", "relay", "recv_p", "recv_m")
    )
    hs, hbuf, ht, wbuf, acch, hret, rbuf = (
        r[k] for k in ("hs", "hbuf", "ht", "wbuf", "acch", "hret", "rbuf")
    )
    saved, pick, pick_t, coef, flip = (r[k] for k in ("saved", "pick", "pick_t", "coef", "flip"))
    xbuf, xfwd, xrel, lsend, lbuf, dpart, dsend, drecv = (
        r[k] for k in ("xbuf", "xfwd", "xrel", "lsend", "lbuf", "dpart", "dsend", "drecv")
    )

    y = lax.axis_index("y")
    xh = lax.axis_index("xh")
    z = lax.axis_index("z")
    xl = lax.axis_index("xl")
    c = lax.axis_index("c")
    x = xh * NXL + xl
    slot = z * 4 + xl * 2 + c
    tok = g_hbm.shape[0]
    half_tok = tok // 2
    topk = ids.shape[0]
    pairs = tok * topk
    frows = ht.shape[0] // NY
    hrow = frows // 2
    hid = w_hbm.shape[0]
    dcols = xbuf.shape[-1]
    drows = drecv.shape[1]
    rows_of = (pl.ds(0, half_tok), pl.ds(half_tok, half_tok))

    def at_x(v):
        return {"xh": v // NXL, "xl": lax.rem(v, NXL)}

    xp, xm, x2 = up(x, 1, NX), up(x, NX - 1, NX), up(x, 2, NX)
    zp, zm, z2 = up(z, 1, NZ), up(z, NZ - 1, NZ), up(z, 2, NZ)
    yp, ym = up(y, 1, NY), up(y, NY - 1, NY)
    dev_x = (at_x(xp), at_x(xm), at_x(x2))
    dev_z = ({"z": zp}, {"z": zm}, {"z": z2})
    dev_y = ({"y": yp}, {"y": ym})
    sibling = {"c": 1 - c}
    classes = {}

    def sems(name, at, out):
        return r["out"].at[classes.setdefault(out, len(classes))], r[name].at[at]

    def remote(src, dst, pair, dev):
        return pltpu.make_async_remote_copy(
            src_ref=src,
            dst_ref=dst,
            send_sem=pair[0],
            recv_sem=pair[1],
            device_id=dev,
            device_id_type=MESH,
        )

    def send(src, dst, pair, dev):
        remote(src, dst, pair, dev).start()

    def arrived(ref, name, at):
        sem = r[name].at[at]
        remote(ref, ref, (sem, sem), sibling).wait_recv()

    def gone(ref, out):
        sem = r["out"].at[classes[out]]
        remote(ref, ref, (sem, sem), sibling).wait_send()

    def plane_dev(n):
        i, j, k = PLANE[n]
        tx, tc, tz = up(x, i, NX), up(c, j, NCORE), up(z, k, NZ)
        return tx, tc, tz, {"xh": tx // NXL, "xl": lax.rem(tx, NXL), "z": tz, "c": tc}

    barrier = pltpu.get_barrier_semaphore()

    def greet():
        for n in range(1, len(PLANE)):
            pl.semaphore_signal(barrier, inc=1, device_id=plane_dev(n)[3], device_id_type=MESH)
        for i in range(1, NY):
            pl.semaphore_signal(barrier, inc=1, device_id={"y": up(y, i, NY)}, device_id_type=MESH)

    def bar():
        pl.semaphore_wait(barrier, len(PLANE) - 1 + NY - 1)

    def own_copy(ch):
        return pltpu.make_async_copy(
            g_hbm.at[:, pl.ds(STARTS[ch], WIDTHS[ch])], gbuf[ch].at[x, c, z], r["loc"].at[0]
        )

    def saved_copy():
        return pltpu.make_async_copy(sv_hbm, saved, r["loc"].at[1])

    def h_local(which):
        lo, hi = PARTS[which]
        col = pl.ds(lo * frows, (hi - lo) * frows)
        return pltpu.make_async_copy(
            hs.at[xh, slot, :, col], hbuf.at[x, c, z, :, col], r["h"].at[which]
        )

    def x_cols(ty, th):
        return x_hbm.at[:, pl.ds(pl.multiple_of((ty * 2 + th) * dcols, 128), dcols)]

    def d_local():
        return pltpu.make_async_copy(x_cols(y, xh), xbuf.at[y, xh], r["dx"].at[0])

    def f_local():
        return pltpu.make_async_copy(x_cols(y, 1 - xh), xfwd.at[y], r["dx"].at[1])

    def w_copy(ch):
        return pltpu.make_async_copy(
            w_hbm.at[:, pl.ds(STARTS[ch], WIDTHS[ch])],
            wbuf.at[ch % 2, :, pl.ds(0, WIDTHS[ch])],
            r["w_sem"].at[ch % 2],
        )

    def prep():
        homes = jnp.zeros(ids.shape, F32)
        for e in range(N_SLOT):
            homes = jnp.where(ids[...] == e, home[e].astype(F32), homes)
        is_live = lax.broadcasted_iota(jnp.int32, ids.shape, 1) < live[0]
        flip[...] = jnp.zeros_like(flip)
        flip[0, 0:topk, 0:tok] = homes
        flip[1, 0:topk, 0:tok] = jnp.where(is_live, gates[...], jnp.zeros_like(gates))
        home_t = flip[0].T[0:tok]
        scale_t = flip[1].T[0:tok]
        lane = lax.broadcasted_iota(jnp.int32, (128, pairs), 1)
        row = lax.broadcasted_iota(jnp.int32, (128, pairs), 0)
        spread = jnp.where(lax.rem(lane, topk) == row, 1.0, 0.0).astype(BF)
        wide = jnp.dot(home_t.astype(BF), spread, preferred_element_type=F32)
        lane = lax.broadcasted_iota(jnp.int32, (tok, pairs), 1)
        row = lax.broadcasted_iota(jnp.int32, (tok, pairs), 0)
        wide = jnp.where(lane // topk == row, wide, -1.0)
        column = lax.broadcasted_iota(jnp.int32, (tok, 128), 1)
        for s in range(N_SLOT):
            pick[s] = jnp.where(wide == float(s), 1.0, 0.0).astype(BF)
            mine = jnp.where((home_t == float(s)) & (column < topk), scale_t, 0.0)
            coef[s] = jnp.broadcast_to(jnp.sum(mine, axis=1, keepdims=True), (tok, 128))
        token = lax.broadcasted_iota(jnp.int32, lat.shape, 0)
        lsend[...] = jnp.where(token < live[0], lat[...], jnp.zeros_like(lat))
        saved_copy().wait()
        table = pick[...].reshape(N_SLOT * tok, pairs)
        scale = coef[...].reshape(N_SLOT * tok, 128)
        for n, k in enumerate(ORDER):
            col = pl.ds(pl.multiple_of(up(y, k, NY) * NXH * frows, NXH * frows), NXH * frows)
            rows = jnp.dot(table, saved[:, col], preferred_element_type=F32)
            for j in range(NXH):
                scaled = (rows[:, j * frows : (j + 1) * frows] * scale).astype(BF)
                hs[j, :, :, n * frows : (n + 1) * frows] = scaled.reshape(N_SLOT, tok, frows)

    def lanes(ch, h):
        return pl.ds(h * (WIDTHS[ch] // 2), WIDTHS[ch] // 2)

    def direct(ch):
        return ch == 0

    def own_wait():
        pltpu.make_async_copy(g_hbm, g_hbm, r["loc"].at[0]).wait()

    def s0(ch):
        for h in range(2):
            ref = gbuf[ch].at[x, c, z, :, lanes(ch, h)]
            for s in range(3 if direct(ch) else 2):
                at = 0 if direct(ch) else ch * 4 + h * 2 + s
                send(ref, ref, sems("a1", at, ("a", ch)), (dev_x, dev_z)[h][s])

    def s1(ch):
        for h in range(2):
            for s in range(2):
                if h == 0:
                    blk = gbuf[ch].at[(xm, xp)[s], c, z]
                else:
                    blk = gbuf[ch].at[x, c, (zm, zp)[s]]
                dev = (dev_x, dev_z)[h][s]
                arrived(blk.at[:, lanes(ch, h)], "a1", ch * 4 + h * 2 + s)
                ref = blk.at[rows_of[s], lanes(ch, h)]
                send(ref, ref, sems("a2", ch, ("a", ch)), dev)

    def line(ch, h, other):
        if h == 0:
            return gbuf[ch].at[:, c, other, :, lanes(ch, 0)]
        return gbuf[ch].at[other, c, :, :, lanes(ch, 1)]

    def line_half(ch, h, other, s):
        if h == 0:
            return gbuf[ch].at[:, c, other, rows_of[s], lanes(ch, 0)]
        return gbuf[ch].at[other, c, :, rows_of[s], lanes(ch, 1)]

    def s2(ch):
        if direct(ch):
            arrived(gbuf[ch].at[0:3, c, z], "a1", 0)
        else:
            arrived(gbuf[ch].at[0, c, z], "a2", ch)
        for h in range(2):
            ref = line(ch, h, (z, x)[h])
            for s in range(2):
                send(ref, ref, sems("b1", ch * 4 + h * 2 + s, ("b", ch)), (dev_z, dev_x)[h][s])
            send(ref, ref, sems("dd", ch, ("d", ch)), sibling)

    def s3(ch):
        for h in range(2):
            for s in range(2):
                other = ((zm, zp), (xm, xp))[h][s]
                dev = (dev_z, dev_x)[h][s]
                ref = line(ch, h, other)
                arrived(ref, "b1", ch * 4 + h * 2 + s)
                fwd = line_half(ch, h, other, s)
                send(fwd, fwd, sems("b2", ch, ("b", ch)), dev)
                send(ref, ref, sems("dd", ch, ("d", ch)), sibling)

    def s4(ch):
        arrived(gbuf[ch].at[:, c, z], "b2", ch)
        for h in range(2):
            ref = line(ch, h, (z2, x2)[h])
            send(ref, ref, sems("dd", ch, ("d", ch)), sibling)

    def s5(ch):
        arrived(gbuf[ch].at[:, 1 - c], "dd", ch)

    def h_send(first, last, which):
        if first == 0:
            h_local(which).start()
        lo, hi = PARTS[which]
        col = pl.ds(lo * frows, (hi - lo) * frows)
        for m in range(first, last):
            n = ((m + 1) * 11) % len(PLANE)
            tx, tc, tz, dev = plane_dev(n)
            t_slot = tz * 4 + lax.rem(tx, NXL) * 2 + tc
            src = hs.at[tx // NXL, t_slot, :, col]
            send(src, hbuf.at[x, c, z, :, col], sems("h", which, "h"), dev)

    def h_build(which):
        lo, hi = PARTS[which]
        col = pl.ds(lo * frows, (hi - lo) * frows)
        arrived(hbuf.at[:, :, :, :, col], "h", which)
        n_tok = NCORE * NZ * tok
        for k in range(lo, hi):
            for i in range(NX):
                blk = hbuf[i, :, :, :, k * frows : (k + 1) * frows].reshape(n_tok, frows)
                ht[pl.ds(k * frows, frows), pl.ds(i * n_tok, n_tok)] = blk.T

    def mm1(ch, lo=0, hi=NY):
        def body(n, carry):
            col = pl.ds(pl.multiple_of(n * 256, 256), 256)
            g = gbuf[ch][:, :, :, :, col].reshape(len(PLANE) * tok, 256)
            p = jnp.dot(ht[lo * frows : hi * frows], g, preferred_element_type=F32)
            for k in range(lo, hi):
                rows = p[(k - lo) * frows : (k - lo + 1) * frows]
                if k == NY - 1:
                    eg_out[:, pl.ds(pl.multiple_of(STARTS[ch] + n * 256, 256), 256)] = rows
                else:
                    part[ch][k, :, col] = rows.astype(BF)
            return carry

        lax.fori_loop(0, WIDTHS[ch] // 256, body, 0)

    def m0(which):
        mm1(0, *PARTS[which])

    def mm2(ch):
        w_copy(ch).wait()

        def body(n, carry):
            row = pl.ds(pl.multiple_of(n * 256, 256), 256)
            g = gbuf[ch][pl.ds(xh * NXL, NXL)].reshape(len(GROUP) * tok, WIDTHS[ch])
            w = wbuf[ch % 2, row, pl.ds(0, WIDTHS[ch])]
            p = lax.dot_general(g, w, (((1,), (1,)), ((), ())), preferred_element_type=F32)
            if ch == 0:
                acch[:, row] = p
            else:
                acch[:, row] = acch[:, row] + p
            return carry

        lax.fori_loop(0, hid // 256, body, 0)
        if ch + 2 < N_CHUNK:
            w_copy(ch + 2).start()

    row_a, row_b = pl.ds(0, hrow), pl.ds(hrow, hrow)

    def r0a(ch):
        p = part[ch]
        send(p.at[0, row_b], relay[ch].at[0], sems("rs", ch * 3 + 0, ("r", ch)), dev_y[0])
        send(p.at[0, row_a], relay[ch].at[1], sems("rs", ch * 3 + 1, ("r", ch)), dev_y[1])

    def r0b(ch):
        p = part[ch]
        send(p.at[1, row_a], recv_m[ch].at[row_a], sems("rs", ch * 3 + 2, ("r", ch)), dev_y[0])
        send(p.at[2, row_b], recv_p[ch].at[row_b], sems("rs", ch * 3 + 2, ("r", ch)), dev_y[1])

    def r1(ch):
        p = part[ch]
        arrived(relay[ch].at[0], "rs", ch * 3)
        p[1, row_b] = (p[1, row_b].astype(F32) + relay[ch][0].astype(F32)).astype(BF)
        send(p.at[1, row_b], recv_m[ch].at[row_b], sems("rs", ch * 3 + 2, ("r", ch)), dev_y[0])
        arrived(relay[ch].at[1], "rs", ch * 3 + 1)
        p[2, row_a] = (p[2, row_a].astype(F32) + relay[ch][1].astype(F32)).astype(BF)
        send(p.at[2, row_a], recv_p[ch].at[row_a], sems("rs", ch * 3 + 2, ("r", ch)), dev_y[1])

    def r2(ch):
        arrived(part[ch].at[0:2], "rs", ch * 3 + 2)
        col = pl.ds(STARTS[ch], WIDTHS[ch])
        eg_out[:, col] = eg_out[:, col] + (recv_m[ch][...].astype(F32) + recv_p[ch][...].astype(F32))

    def group_dev(n):
        i, j, k = GROUP[n]
        tx, tc, tz = up(xl, i, NXL), up(c, j, NCORE), up(z, k, NZ)
        return tx, tc, tz, {"xl": tx, "z": tz, "c": tc}

    def hr_send():
        hret[...] = acch[...].astype(BF).reshape(hret.shape)
        for n in range(1, len(GROUP)):
            tx, tc, tz, dev = group_dev(n)
            send(hret.at[tx, tc, tz], rbuf.at[slot], sems("hr", 0, "hr"), dev)
        pltpu.make_async_copy(hret.at[xl, c, z], rbuf.at[slot], r["hr"].at[0]).start()

    def table_flip():
        pick_t[...] = pick[...].reshape(N_SLOT * tok, pairs).T

    def hr_wait():
        arrived(rbuf, "hr", 0)
        scale = coef[...].reshape(N_SLOT * tok, 128)
        for n in range(hid // 256):
            halves = []
            for j in range(2):
                rows = rbuf[:, :, n * 256 + j * 128 : n * 256 + (j + 1) * 128]
                rows = rows.reshape(N_SLOT * tok, 128).astype(F32) * scale
                halves.append(rows.astype(BF))
            rows = jnp.concatenate(halves, axis=1)
            back = jnp.dot(pick_t[...], rows, preferred_element_type=F32)
            hg_out[:, n * 256 : (n + 1) * 256] = back.astype(BF)

    def d0a():
        d_local().start()
        f_local().start()
        lbuf[y, xh] = lsend[...]
        for i in range(1, NY):
            ty = up(y, i, NY)
            dev = {"y": ty}
            send(x_cols(ty, 1 - xh), xfwd.at[y], sems("dx", 1, "dx"), dev)
            send(lsend, lbuf.at[y, xh], sems("dl", 0, "dl"), dev)
            send(x_cols(ty, xh), xbuf.at[y, xh], sems("dx", 0, "dx"), dev)

    def d0b():
        arrived(xfwd, "dx", 1)
        arrived(lbuf.at[0:3, xh], "dl", 0)
        for s in range(2):
            send(xfwd.at[2 * s : 2 * s + 2], xrel.at[s], sems("xr", s, "dxf"), dev_x[s])
        send(lbuf.at[:, xh], lbuf.at[:, xh], sems("dl", 1, "dlf"), {"xh": 1 - xh})

    def d0c():
        for s in range(2):
            arrived(xrel.at[s], "xr", s)
            dst = xbuf.at[pl.ds(2 * s, 2), (xm, xp)[s] // NXL]
            send(xrel.at[s], dst, sems("dx", 0, "dxf"), dev_x[s])

    def d1():
        arrived(xbuf, "dx", 0)
        arrived(lbuf.at[:, xh], "dl", 1)
        n_tok = NY * NXH * tok

        def body(n, carry):
            col = pl.ds(pl.multiple_of(n * 128, 128), 128)
            xt = xbuf[:, :, :, col].reshape(n_tok, 128).T
            dpart[col, :] = jnp.dot(
                xt, lbuf[...].reshape(n_tok, lbuf.shape[-1]), preferred_element_type=F32
            )
            return carry

        lax.fori_loop(0, dcols // 128, body, 0)
        for n in range(N_SLOT):
            dsend[n] = dpart[n * drows : (n + 1) * drows].astype(BF)
        for n in range(1, len(GROUP)):
            tx, tc, tz, dev = group_dev(n)
            send(dsend.at[tz * 4 + tx * 2 + tc], drecv.at[slot], sems("ds", 0, "ds"), dev)
        pltpu.make_async_copy(dsend.at[slot], drecv.at[slot], r["ds"].at[0]).start()

    def d2():
        arrived(drecv, "ds", 0)
        mine = dpart[pl.ds(pl.multiple_of(slot * drows, 8), drows)]
        total = mine - drecv[slot].astype(F32)
        for n in range(len(GROUP)):
            total = total + drecv[n].astype(F32)
        dg_out[...] = total

    def sendwait():
        for ch in range(N_CHUNK):
            gone(gbuf[ch].at[0:3, c, z], ("a", ch))
            gone(gbuf[ch].at[0:3, c], ("b", ch))
            gone(gbuf[ch].at[:, c], ("d", ch))
            gone(part[ch], ("r", ch))
        gone(ht.at[0 : ht.shape[0] // 32 * 31], "h")
        gone(wbuf.at[0, pl.ds(0, (len(GROUP) - 1) * tok), pl.ds(0, hid)], "hr")
        gone(dsend.at[0 : N_SLOT - 1], "ds")
        gone(xbuf.at[0:3], "dx")
        gone(xbuf, "dxf")
        gone(lbuf.at[0:3, xh], "dl")
        gone(lbuf.at[:, xh], "dlf")

    greet()
    saved_copy().start()
    own_copy(0).start()
    own_copy(1).start()
    own_copy(2).start()
    own_copy(3).start()
    own_copy(4).start()
    w_copy(0).start()
    w_copy(1).start()
    prep()
    own_wait()
    bar()
    s0(0)
    h_send(0, 8, 0)
    h_send(8, 16, 0)
    h_send(16, 24, 0)
    h_send(24, 31, 0)
    s0(1)
    d0a()
    table_flip()
    s2(0)
    h_send(0, 8, 1)
    h_send(8, 16, 1)
    h_send(16, 24, 1)
    s0(2)
    s1(1)
    s3(0)
    h_send(24, 31, 1)
    s4(0)
    s2(1)
    h_send(0, 8, 2)
    h_send(8, 16, 2)
    h_build(0)
    s5(0)
    m0(0)
    r0a(0)
    h_build(1)
    m0(1)
    r0b(0)
    s1(2)
    h_send(16, 24, 2)
    h_send(24, 31, 2)
    s3(1)
    s0(3)
    s2(2)
    mm2(0)
    s0(4)
    s4(1)
    h_build(2)
    r1(0)
    s5(1)
    mm1(1)
    s1(3)
    r0a(1)
    s3(2)
    s1(4)
    s2(3)
    r0b(1)
    mm2(1)
    s4(2)
    r1(1)
    m0(2)
    r2(0)
    s2(4)
    s5(2)
    mm1(2)
    s3(3)
    r0a(2)
    r0b(2)
    mm2(2)
    s4(3)
    s3(4)
    d0b()
    s5(3)
    mm1(3)
    r0a(3)
    r0b(3)
    s4(4)
    d0c()
    mm2(3)
    s5(4)
    mm1(4)
    r0a(4)
    r0b(4)
    mm2(4)
    hr_send()
    r1(2)
    d1()
    r1(3)
    r2(1)
    r2(2)
    r1(4)
    r2(3)
    d2()
    hr_wait()
    r2(4)
    sendwait()


def exchange(ids, home, live, gates, lat, g, sv, w, xin):
    tok, d = g.shape
    pairs, hid = sv.shape
    kvr = lat.shape[1]
    frows = hid // 8
    drows = d // 128
    dma = pltpu.SemaphoreType.DMA
    v = pltpu.VMEM
    smem, vmem, hbm = (
        pl.BlockSpec(memory_space=m) for m in (pltpu.SMEM, pltpu.VMEM, pl.ANY)
    )
    ins = {
        "ids": vmem, "home": smem, "live": smem, "gates": vmem, "lat": vmem,
        "g": hbm, "sv": hbm, "w": hbm, "x": hbm,
    }
    outs = ("hg_out", "eg_out", "dg_out")
    scratch = {
        "hs": v((NXH, N_SLOT, tok, hid // NXH), BF),
        "hbuf": v((NX, NCORE, NZ, tok, hid // NXH), BF),
        "ht": v((hid // NXH, len(PLANE) * tok), BF),
        "wbuf": v((2, hid, max(WIDTHS)), BF),
        "acch": v((len(GROUP) * tok, hid), F32),
        "hret": v((NXL, NCORE, NZ, tok, hid), BF),
        "rbuf": v((N_SLOT, tok, hid), BF),
        "saved": v((pairs, hid), BF),
        "pick": v((N_SLOT, tok, pairs), BF),
        "pick_t": v((pairs, N_SLOT * tok), BF),
        "coef": v((N_SLOT, tok, 128), F32),
        "flip": v((2, 128, 128), F32),
        "xbuf": v((NY, NXH, tok, d // 8), BF),
        "xfwd": v((NY, tok, d // 8), BF),
        "xrel": v((2, NY // 2, tok, d // 8), BF),
        "lsend": v((tok, kvr), BF),
        "lbuf": v((NY, NXH, tok, kvr), BF),
        "dpart": v((d // 8, kvr), F32),
        "dsend": v((N_SLOT, drows, kvr), BF),
        "drecv": v((N_SLOT, drows, kvr), BF),
    }
    for i, width in enumerate(WIDTHS):
        scratch["gbuf" + str(i)] = v((NX, NCORE, NZ, tok, width), BF)
        scratch["part" + str(i)] = v((NY - 1, frows, width), BF)
        scratch["relay" + str(i)] = v((2, frows // 2, width), BF)
        scratch["recv_p" + str(i)] = v((frows, width), BF)
        scratch["recv_m" + str(i)] = v((frows, width), BF)
    counts = {
        "a1": N_CHUNK * 4, "a2": N_CHUNK, "b1": N_CHUNK * 4, "b2": N_CHUNK, "dd": N_CHUNK,
        "h": len(PARTS), "rs": N_CHUNK * 3, "hr": 1, "dx": 2, "xr": 2, "dl": 2, "ds": 1,
        "loc": 2, "w_sem": 2, "out": N_CHUNK * 4 + 7,
    }
    for name, count in counts.items():
        scratch[name] = dma((count,))
    names = tuple(ins) + outs + tuple(scratch)

    def body(*refs):
        kernel(names, *refs)

    return pl.pallas_call(
        body,
        out_shape=(
            v((pairs, hid), BF),
            v((frows, d), F32),
            v((drows, kvr), F32),
        ),
        in_specs=list(ins.values()),
        out_specs=(vmem, vmem, vmem),
        scratch_shapes=list(scratch.values()),
        compiler_params=pltpu.CompilerParams(
            collective_id=0, has_side_effects=True, vmem_limit_bytes=56 * 1024 * 1024
        ),
        name="exchange",
    )(ids, home, live, gates, lat, g, sv, w, xin)


def leave(hg, eg, dg):
    pieces = 4
    step = eg.shape[0] // pieces

    def body(hg_in, eg_in, dg_in, hg_out, eg_out, dg_out, sem):
        copies = [
            pltpu.make_async_copy(
                eg_in.at[pl.ds(i * step, step)], eg_out.at[pl.ds(i * step, step)], sem.at[i]
            )
            for i in range(pieces)
        ]
        copies.append(pltpu.make_async_copy(hg_in, hg_out, sem.at[pieces]))
        copies.append(pltpu.make_async_copy(dg_in, dg_out, sem.at[pieces + 1]))
        for copy in copies:
            copy.start()
        for copy in copies:
            copy.wait()

    return pl.pallas_call(
        body,
        out_shape=tuple(jax.ShapeDtypeStruct(a.shape, a.dtype) for a in (hg, eg, dg)),
        in_specs=[pl.BlockSpec(memory_space=pltpu.VMEM)] * 3,
        out_specs=(pl.BlockSpec(memory_space=pl.ANY),) * 3,
        scratch_shapes=[pltpu.SemaphoreType.DMA((pieces + 2,))],
        compiler_params=pltpu.CompilerParams(vmem_limit_bytes=1024 * 1024),
        name="leave",
    )(hg, eg, dg)


def on_device(
    expert_ids,
    expert_home,
    live_tokens,
    gate_weights,
    output_grad,
    saved_hidden,
    down_weight,
    dense_input,
    latent_grad,
):
    tok, topk = expert_ids.shape
    hid = saved_hidden.shape[2]
    hg, eg, dg = exchange(
        expert_ids.T,
        expert_home,
        live_tokens,
        gate_weights.T,
        latent_grad,
        output_grad,
        saved_hidden.reshape(tok * topk, hid),
        down_weight[0],
        dense_input,
    )
    hg, eg, dg = leave(hg, eg, dg)
    return hg.reshape(tok, topk, hid), eg[None], dg


def solution(mesh):
    torus = Mesh(mesh.devices.reshape(4, 2, 4, 2, 2), ALL)
    in_specs = (
        P(ALL, None),
        P(),
        P(ALL),
        P(ALL, None),
        P(ALL, None),
        P(ALL, None, None),
        P(EXPERT, None, None),
        P(ALL, None),
        P(ALL, None),
    )
    out_specs = (P(ALL, None, None), P(EXPERT, DP, None), P(ALL, None))
    return jax.shard_map(
        on_device, mesh=torus, in_specs=in_specs, out_specs=out_specs, check_vma=False
    )
```
